32 devices in a mesh: rows: 32 (over z, y, x, core).
Axes of the slice: x: 2, y: 2, z: 4, core: 2. Of those that a mesh axis runs over, the one named last changes fastest.
Arguments:
- right_sides: float32 [32, 32768], P(None, 'rows'), may hold values from -48 to 48
- initial: float32 [32, 32768], P(None, 'rows'), may hold values from -1.2 to 1.2
- diag_blocks: float32 [32768, 256], P('rows'), may hold values from -2 to 9
- sub_blocks: float32 [32768, 256], P('rows'), may hold values from -0.21875 to 0.21875
- super_blocks: float32 [32768, 256], P('rows'), may hold values from -0.21875 to 0.21875
- local_inverse: bfloat16 [32768, 1024], P('rows'), may hold values from -1 to 1
- upper_spikes: bfloat16 [256, 32768], P(None, 'rows'), may hold values from -0.21875 to 0.21875
- lower_spikes: bfloat16 [256, 32768], P(None, 'rows'), may hold values from -2 to 2
Outputs:
- solution: float32 [32, 32768], P(None, 'rows')
- residual_norms: float32 [3, 32], replicated
The draws below stay inside these ranges and needn't reach their ends.
All inputs are finite; a program needn't handle non-finite values.
Results may differ from the reference program's by a relative error of at most 0.002.
The reference program's roundings to bfloat16 on the way (of `rounded`) count: a program that leaves them out, or rounds other values in their place, can miss the bound.
Values may be sent and summed in bfloat16 or wider, within the bound.
No kernel may reach another device: no remote copies, remote signals or barrier semaphores. Data moves between devices by JAX's collectives and lax.ppermute only.
A program may use at most 64 MiB of HBM per device.

```python
import math
import jax
import jax.numpy as jnp
from jax import lax

BAND = 256
RHS = 32
ROWS_DEV = 1024
ITERS = 2
ORDER = 32768
N_ROWS = 32


def block_parts(key):
    base_key = jax.random.fold_in(key, 101)
    block_total = ORDER // BAND
    log_scales = jax.random.uniform(jax.random.fold_in(base_key, 1), (block_total, BAND), jnp.float32, math.log(2.0), math.log(8.0))
    mixing = jnp.clip(jax.random.normal(jax.random.fold_in(base_key, 2), (block_total, BAND, BAND), jnp.float32), -5.0, 5.0)
    return (jnp.exp(log_scales), mixing * (0.3 / math.sqrt(BAND)))


def draw_diag_blocks(key, part):
    scales, mixing = block_parts(key)
    unit_matrix = jnp.eye(BAND, dtype=jnp.float32)
    blocks = mixing + scales[:, :, None] * unit_matrix[None]
    return blocks.reshape(ORDER, BAND)


def draw_local_inverse(key, part):
    scales, mixing = block_parts(key)
    inverse_scale = 1.0 / scales
    unit_matrix = jnp.eye(BAND, dtype=jnp.float32)
    approx = inverse_scale[:, :, None] * unit_matrix[None] - inverse_scale[:, :, None] * mixing * inverse_scale[:, None, :]
    per_device = ROWS_DEV // BAND
    approx = approx.reshape(N_ROWS, per_device, BAND, BAND)
    positioned_rows = jnp.einsum('pkij,kl->pkilj', approx, jnp.eye(per_device, dtype=jnp.float32))
    noise = jnp.clip(jax.random.normal(jax.random.fold_in(key, 102), (N_ROWS, ROWS_DEV, ROWS_DEV), jnp.float32), -5.0, 5.0)
    whole = positioned_rows.reshape(N_ROWS, ROWS_DEV, ROWS_DEV) + noise * (0.06 / math.sqrt(ROWS_DEV))
    return jnp.clip(whole.reshape(ORDER, ROWS_DEV), -1.0, 1.0).astype(jnp.bfloat16)


def draw_lower_spikes(key, part):
    inner = jnp.clip(jax.random.normal(jax.random.fold_in(key, 21), (BAND, N_ROWS, ROWS_DEV - BAND), jnp.float32), -5.0, 5.0)
    inner = inner * (0.3 / math.sqrt(BAND))
    slow_share = 0.5
    slowness = jax.random.uniform(jax.random.fold_in(key, 22), (BAND,), jnp.float32) < slow_share
    fast_rate = jnp.exp(jax.random.uniform(jax.random.fold_in(key, 23), (BAND,), jnp.float32, math.log(0.15), math.log(1.0)))
    rates = jnp.where(slowness, 2.5 / N_ROWS, fast_rate)
    spread = jax.random.uniform(jax.random.fold_in(key, 24), (N_ROWS, BAND), jnp.float32, 0.6, 1.4)
    retain = jnp.exp(-rates[None, :] * spread)
    spike_position = jax.random.randint(jax.random.fold_in(key, 25), (3,), 0, N_ROWS)
    eliminated_rows = jnp.any(jnp.arange(N_ROWS)[:, None] == spike_position[None, :], axis=1)
    retain = jnp.where(eliminated_rows[:, None] & slowness[None, :], retain * 0.6, retain)
    mixing = jnp.clip(jax.random.normal(jax.random.fold_in(key, 26), (N_ROWS, BAND, BAND), jnp.float32), -5.0, 5.0)
    coupling = jnp.eye(BAND, dtype=jnp.float32)[None] + mixing * (0.2 / math.sqrt(BAND))
    tip_blocks = -(coupling * retain[:, None, :])
    tip_layout = jnp.transpose(tip_blocks, (1, 0, 2))
    whole = jnp.concatenate([inner, tip_layout], axis=2)
    return jnp.clip(whole.reshape(BAND, ORDER), -2.0, 2.0).astype(jnp.bfloat16)


def draw_right_sides(key, part):
    column = jnp.arange(ORDER, dtype=jnp.float32) / ORDER
    jitter = jax.random.uniform(jax.random.fold_in(key, 31), (ORDER,), jnp.float32, -1.15, 1.15)
    rough = jnp.clip(jax.random.normal(jax.random.fold_in(key, 34), (RHS, ORDER), jnp.float32), -4.0, 4.0)
    column_scale = jnp.exp(math.log(3.0) * column + jitter)
    values = rough * column_scale[None, :]
    return jnp.clip(values, -48.0, 48.0)


def block_levels(stream_key, dims, split, smallest, largest):
    gain = 1.0
    for axis_at, shards_of in split:
        steps = jax.random.uniform(jax.random.fold_in(jax.random.fold_in(stream_key, 6), axis_at), (shards_of,), jnp.float32, smallest / len(split), largest / len(split))
        gain = gain * jnp.repeat(jnp.exp(steps), dims[axis_at] // shards_of).reshape((-1,) + (1,) * (len(dims) - 1 - axis_at))
    return gain


def gaussian(stream_key, extent, width, reach, cuts=(), held_as=jnp.bfloat16):
    loudness = block_levels(stream_key, extent, cuts, -0.22, 0.18) if cuts else 1.0
    entries = jax.random.normal(stream_key, extent, jnp.float32) * width * loudness
    return jnp.minimum(jnp.maximum(entries, -reach), reach).astype(held_as)


def setup_inputs(seed: int = 0) -> dict:
    splits = jax.random.split(jax.random.key(seed), 9)
    return {
        "right_sides": draw_right_sides(jax.random.fold_in(splits[8], 71), 0),
        "initial": gaussian(splits[1], (RHS, ORDER), 0.2, 1.2, ((1, 32),), jnp.float32),
        "diag_blocks": draw_diag_blocks(jax.random.fold_in(splits[8], 71), 0),
        "sub_blocks": gaussian(splits[3], (ORDER, BAND), (3 * BAND) ** -0.5, 0.21875, ((0, 32),), jnp.float32),
        "super_blocks": gaussian(splits[4], (ORDER, BAND), (3 * BAND) ** -0.5, 0.21875, ((0, 32),), jnp.float32),
        "local_inverse": draw_local_inverse(jax.random.fold_in(splits[8], 71), 0),
        "upper_spikes": gaussian(splits[6], (BAND, ORDER), (3 * BAND) ** -0.5, 0.21875, ((1, 32),)),
        "lower_spikes": draw_lower_spikes(jax.random.fold_in(splits[8], 71), 0),
    }


maximum_level = lax.Precision.HIGHEST

def residual_of(right_sides, solution, diag_mat, lower_mat, upper_mat):
    padded = jnp.pad(solution, ((0, 0), (BAND, BAND)))
    stacked = padded.reshape(padded.shape[0], -1, BAND)
    applied = jnp.einsum('rkb,kbc->rkc', stacked[:, 1:-1], diag_mat, precision=maximum_level)
    applied = applied + jnp.einsum('rkb,kbc->rkc', stacked[:, :-2], lower_mat, precision=maximum_level)
    applied = applied + jnp.einsum('rkb,kbc->rkc', stacked[:, 2:], upper_mat, precision=maximum_level)
    return right_sides - applied.reshape(right_sides.shape)

def norm_row(residual):
    return jnp.sqrt(lax.optimization_barrier(jnp.sum(residual * residual, axis=1)) / ORDER)

def solve_partition(operands):
    return jnp.dot(operands[0].astype(jnp.float32), operands[1].astype(jnp.float32), precision=maximum_level)

def advance(carried, operands):
    current = operands[0] + jnp.dot(carried, operands[1], precision=maximum_level)
    return (current, (carried, current))

def rounded_copy(values):
    return lax.optimization_barrier(values.astype(jnp.bfloat16)).astype(jnp.float32)

def reference(right_sides, initial, diag_blocks, sub_blocks, super_blocks, local_inverse, upper_spikes, lower_spikes):
    diag_mat = diag_blocks.reshape(-1, BAND, BAND)
    lower_mat = sub_blocks.reshape(-1, BAND, BAND)
    upper_mat = super_blocks.reshape(-1, BAND, BAND)
    inverse_parts = local_inverse.reshape(N_ROWS, ROWS_DEV, ROWS_DEV)
    upper_pieces = upper_spikes.reshape(BAND, N_ROWS, ROWS_DEV).astype(jnp.float32)
    lower_pieces = lower_spikes.reshape(BAND, N_ROWS, ROWS_DEV).astype(jnp.float32)
    chain_mats = -jnp.transpose(lower_pieces[:, :, ROWS_DEV - BAND:], (1, 0, 2))
    bottom_upper = jnp.transpose(upper_pieces[:, :, ROWS_DEV - BAND:], (1, 0, 2))
    top_lower = jnp.transpose(lower_pieces[:, :, :BAND], (1, 0, 2))
    next_lower = jnp.concatenate([top_lower[1:], jnp.zeros_like(top_lower[:1])], axis=0)
    solution = initial
    records = []
    for turn_index in range(ITERS):
        residual = residual_of(right_sides, solution, diag_mat, lower_mat, upper_mat)
        records.append(norm_row(residual))
        rounded = residual.astype(jnp.bfloat16).reshape(RHS, N_ROWS, ROWS_DEV).transpose(1, 0, 2)
        local_part = lax.map(solve_partition, (rounded, inverse_parts))
        own_top = local_part[:, :, :BAND]
        next_top = jnp.concatenate([own_top[1:], jnp.zeros_like(own_top[:1])], axis=0)
        offset = local_part[:, :, ROWS_DEV - BAND:] - jnp.einsum('pri,pij->prj', next_top, bottom_upper, precision=maximum_level)
        leftover, outputs = lax.scan(advance, jnp.zeros((RHS, BAND), jnp.float32), (offset, chain_mats))
        previous, current = outputs
        top_tip = next_top - jnp.einsum('pri,pij->prj', current, next_lower, precision=maximum_level)
        correction = local_part - jnp.einsum('pri,ipm->prm', rounded_copy(top_tip), upper_pieces, precision=maximum_level)
        correction = correction - jnp.einsum('pri,ipm->prm', rounded_copy(previous), lower_pieces, precision=maximum_level)
        solution = solution + correction.transpose(1, 0, 2).reshape(RHS, ORDER)
    residual = residual_of(right_sides, solution, diag_mat, lower_mat, upper_mat)
    records.append(norm_row(residual))
    return (solution, jnp.stack(records))
```

```python
import jax
import jax.numpy as jnp
from jax import lax
from jax.sharding import PartitionSpec as P

ITERS = 2
AXIS = "rows"
HIGHEST = lax.Precision.HIGHEST


def exact(left, right):
    return jnp.dot(left, right, precision=HIGHEST, preferred_element_type=jnp.float32)


def mixed(left, right):
    return jnp.dot(left, right, preferred_element_type=jnp.float32)


def exchange(values, distance):
    count = lax.axis_size(AXIS)
    return lax.ppermute(values, AXIS, [(i, i ^ distance) for i in range(count)])


def across(values):
    count = lax.axis_size(AXIS)
    pairs = [(i, i + 1) for i in range(1, count - 1, 2)]
    return lax.ppermute(values, AXIS, pairs + [(b, a) for a, b in pairs])


def neighbours(to_left, to_right, even):
    near = exchange(jnp.where(even, to_right, to_left), 1)
    far = across(jnp.where(even, to_left, to_right))
    return jnp.where(even, far, near), jnp.where(even, near, far)


def blocks_of(matrix, width):
    return [matrix[i : i + width] for i in range(0, matrix.shape[0], width)]


def body(
    right_sides,
    initial,
    diag_blocks,
    sub_blocks,
    super_blocks,
    local_inverse,
    upper_spikes,
    lower_spikes,
):
    width = diag_blocks.shape[1]
    count = lax.axis_size(AXIS)
    here = lax.axis_index(AXIS)
    even = here % 2 == 0
    levels = (count - 1).bit_length()
    order_total = right_sides.shape[1] * count
    diag = blocks_of(diag_blocks, width)
    sub = blocks_of(sub_blocks, width)
    sup = blocks_of(super_blocks, width)
    last = len(diag) - 1

    def columns(values, k):
        return values[:, k * width : (k + 1) * width]

    def residual_of(solution, from_left, from_right):
        x = [columns(solution, k) for k in range(last + 1)]
        parts = []
        for k in range(last + 1):
            part = columns(right_sides, k) - exact(x[k], diag[k])
            if k > 0:
                part = part - exact(x[k - 1], sub[k])
            if k < last:
                part = part - exact(x[k + 1], sup[k])
            parts.append(part)
        parts[0] = parts[0] - exact(from_left, sub[0])
        parts[last] = parts[last] - exact(from_right, sup[last])
        return jnp.concatenate(parts, axis=1)

    def halo(solution):
        return neighbours(columns(solution, 0), columns(solution, last), even)

    own_chain = -columns(lower_spikes, last)
    from_left, from_right = halo(initial)
    upper_before, lower_after = neighbours(
        columns(lower_spikes, 0), columns(upper_spikes, last), even
    )
    upper_before = upper_before.astype(jnp.float32)
    lower_after = lower_after.astype(jnp.float32)
    bottom_upper = columns(upper_spikes, last).astype(jnp.float32)
    chain = own_chain.astype(jnp.float32)
    tip_mix = exact(upper_before, chain)

    level_mats = []
    whole = chain
    prefix = None
    for level in range(levels):
        distance = 1 << level
        right = (here & distance) != 0
        if level == levels - 1:
            level_mats.append((right, None if prefix is None else jnp.where(right, prefix, 0.0), None))
            break
        if level == 0:
            other = exchange(own_chain, 1).astype(jnp.float32)
        else:
            half = width // 2
            odd_half = jnp.where(even, whole[:half], whole[half:])
            got = exchange(odd_half, distance)
            twin = exchange(got, 1)
            other = jnp.where(
                even, jnp.concatenate([got, twin], 0), jnp.concatenate([twin, got], 0)
            )
        second = jnp.where(right, whole, other)
        first = jnp.where(right, other, whole)
        level_mats.append((right, None if prefix is None else jnp.where(right, prefix, 0.0), second))
        if prefix is None:
            prefix = jnp.where(right, other, jnp.eye(width, dtype=jnp.float32))
        else:
            prefix = jnp.where(right, exact(first, prefix), prefix)
        whole = exact(first, second)

    partials = []
    solution = initial
    for turn in range(ITERS):
        residual = residual_of(solution, from_left, from_right)
        partials.append(jnp.sum(residual * residual, axis=1))
        local = mixed(residual.astype(jnp.bfloat16), local_inverse)
        own_top = columns(local, 0)
        own_bottom = columns(local, last)
        total = own_bottom - exact(own_top, tip_mix)
        carry = None
        far_top = across(own_top)
        for level, (right, reach, second) in enumerate(level_mats):
            if level == 0:
                both = exchange(jnp.concatenate([total, own_top], 0), 1)
                got, near_top = both[: total.shape[0]], both[total.shape[0] :]
                carry = jnp.where(right, got, 0.0)
            else:
                got = exchange(total, 1 << level)
                carry = carry + exact(got, reach)
            if second is not None:
                total = exact(jnp.where(right, got, total), second) + jnp.where(right, total, got)
        next_top = jnp.where(even, near_top, far_top)
        previous = carry - exact(own_top, upper_before)
        bottom = own_bottom - exact(next_top, bottom_upper) + exact(previous, chain)
        top = next_top - exact(bottom, lower_after)
        correction = local - mixed(top.astype(jnp.bfloat16), upper_spikes)
        correction = correction - mixed(previous.astype(jnp.bfloat16), lower_spikes)
        solution = solution + correction
        from_left, from_right = halo(solution)
    residual = residual_of(solution, from_left, from_right)
    partials.append(jnp.sum(residual * residual, axis=1))
    mine = jnp.concatenate(partials)[None]
    gathered = lax.all_to_all(jnp.broadcast_to(mine, (count, mine.shape[1])), AXIS, 0, 0)
    totals = jnp.sum(gathered, axis=0).reshape(ITERS + 1, right_sides.shape[0])
    return (solution, jnp.sqrt(totals / order_total))


def solution(mesh):
    return jax.shard_map(
        body,
        mesh=mesh,
        in_specs=(
            P(None, AXIS),
            P(None, AXIS),
            P(AXIS, None),
            P(AXIS, None),
            P(AXIS, None),
            P(AXIS, None),
            P(None, AXIS),
            P(None, AXIS),
        ),
        out_specs=(P(None, AXIS), P()),
        check_vma=False,
    )
```

```python
import functools

import jax
import jax.numpy as jnp
from jax import lax
from jax.experimental import pallas as pl
from jax.experimental.pallas import tpu as pltpu
from jax.sharding import PartitionSpec as P

ITERS = 2
AXIS = "rows"
F32 = jnp.float32
BF16 = jnp.bfloat16


def exchange(values, distance):
    count = lax.axis_size(AXIS)
    return lax.ppermute(values, AXIS, [(i, i ^ distance) for i in range(count)])


def across(values):
    count = lax.axis_size(AXIS)
    pairs = [(i, i + 1) for i in range(1, count - 1, 2)]
    return lax.ppermute(values, AXIS, pairs + [(b, a) for a, b in pairs])


def kernel_call(kernel, outs, *args, scalars=1):
    specs = [pl.BlockSpec(memory_space=pltpu.SMEM)] * scalars
    specs += [pl.BlockSpec(memory_space=pltpu.VMEM)] * (len(args) - scalars)
    return pl.pallas_call(
        kernel,
        in_specs=specs,
        out_specs=[pl.BlockSpec(memory_space=pltpu.VMEM)] * len(outs),
        out_shape=[pltpu.VMEM(shape, dtype) for shape, dtype in outs],
        compiler_params=pltpu.CompilerParams(vmem_limit_bytes=16 * 2**20),
    )(*args)


def split3(values):
    high = values.astype(BF16)
    rest = values - high.astype(F32)
    mid = rest.astype(BF16)
    low = (rest - mid.astype(F32)).astype(BF16)
    return high, mid, low


def dot(left, right):
    return jnp.dot(left, right, preferred_element_type=F32)


def fold(product, count):
    rows = product.shape[0] // count
    total = product[(count - 1) * rows :]
    for i in range(count - 2, -1, -1):
        total = total + product[i * rows : (i + 1) * rows]
    return total


def times_exact(parts, right):
    return fold(dot(jnp.concatenate(parts, 0), right), 3)


def times_split(parts, high, mid, low):
    small = dot(parts[0], low) + fold(dot(jnp.concatenate(parts[:2], 0), mid), 2)
    return fold(dot(jnp.concatenate(parts, 0), high), 3) + small


def payload_kernel(even_ref, x_ref, u_ref, l_ref, xn_ref, xf_ref, sn_ref, sf_ref, chain_ref):
    even = even_ref[0] == 1
    width = xn_ref.shape[1]
    first, final = x_ref[:, :width], x_ref[:, -width:]
    xn_ref[...] = jnp.where(even, final, first)
    xf_ref[...] = jnp.where(even, first, final)
    low_tip, up_tip = l_ref[:, :width].astype(F32), u_ref[:, -width:].astype(F32)
    sn_ref[...] = jnp.where(even, up_tip, low_tip).astype(BF16)
    sf_ref[...] = jnp.where(even, low_tip, up_tip).astype(BF16)
    chain_ref[...] = -l_ref[:, -width:]


def split_store(ref, k, width, values):
    for j, part in enumerate(split3(values)):
        ref[j, pl.ds(k * width, width), :] = part


def first_local_kernel(b_ref, x_ref, d_ref, s_ref, p_ref, acc_ref, d3_ref, s3_ref, p3_ref):
    width = d_ref.shape[1]
    for k in range(d_ref.shape[0] // width):
        rows = pl.ds(k * width, width)
        split_store(d3_ref, k, width, d_ref[rows, :])
        split_store(s3_ref, k, width, s_ref[rows, :])
        split_store(p3_ref, k, width, p_ref[rows, :])
    local_part(b_ref, x_ref, d3_ref, s3_ref, p3_ref, acc_ref)


def local_part(b_ref, x_ref, d3_ref, s3_ref, p3_ref, acc_ref):
    width = d3_ref.shape[2]
    last = d3_ref.shape[1] // width - 1
    x = [split3(x_ref[:, k * width : (k + 1) * width]) for k in range(last + 1)]
    for k in range(last + 1):
        rows = pl.ds(k * width, width)
        part = times_split(x[k], *(d3_ref[j, rows, :] for j in range(3)))
        if k > 0:
            part = part + times_split(x[k - 1], *(s3_ref[j, rows, :] for j in range(3)))
        if k < last:
            part = part + times_split(x[k + 1], *(p3_ref[j, rows, :] for j in range(3)))
        acc_ref[:, k * width : (k + 1) * width] = b_ref[:, k * width : (k + 1) * width] - part


def close_residual(even_ref, acc_ref, near_ref, far_ref, s3_ref, p3_ref):
    even = even_ref[0] == 1
    width = s3_ref.shape[2]
    last = s3_ref.shape[1] - width
    near, far = near_ref[...], far_ref[...]
    before = split3(jnp.where(even, far, near))
    after = split3(jnp.where(even, near, far))
    first = acc_ref[:, :width] - times_split(before, *(s3_ref[j, :width, :] for j in range(3)))
    final = acc_ref[:, last:] - times_split(after, *(p3_ref[j, last:, :] for j in range(3)))
    return first, acc_ref[:, width:last], final


def squares(parts):
    return sum(jnp.sum(p * p, axis=1, keepdims=True) for p in parts)


def solve_kernel(even_ref, acc_ref, near_ref, far_ref, s3_ref, p3_ref, z_ref, mix_ref, both_ref, local_ref, norm_ref):
    parts = close_residual(even_ref, acc_ref, near_ref, far_ref, s3_ref, p3_ref)
    norm_ref[...] = squares(parts)
    width = s3_ref.shape[2]
    rows = acc_ref.shape[0]
    rounded = jnp.concatenate([p.astype(BF16) for p in parts], 1)
    local = dot(rounded, z_ref[...])
    local_ref[...] = local
    own_top = local[:, :width]
    mixed = times_split(split3(own_top), *(mix_ref[j] for j in range(3)))
    both_ref[:rows, :] = local[:, -width:] - mixed
    both_ref[rows:, :] = own_top


def norm_kernel(even_ref, acc_ref, near_ref, far_ref, s3_ref, p3_ref, norm_ref):
    norm_ref[...] = squares(close_residual(even_ref, acc_ref, near_ref, far_ref, s3_ref, p3_ref))


def mix_kernel(even_ref, near_ref, far_ref, chain_ref, before_ref, after_ref, mix_ref):
    even = even_ref[0] == 1
    near, far = near_ref[...].astype(F32), far_ref[...].astype(F32)
    before = jnp.where(even, far, near).astype(BF16)
    before_ref[...] = before
    after_ref[...] = jnp.where(even, near, far).astype(BF16)
    for j, part in enumerate(split3(dot(before, chain_ref[...]))):
        mix_ref[j] = part


def start_static_kernel(right_ref, own_ref, other_ref, whole_ref, half_ref, second_ref, prefix_ref):
    right = right_ref[0] == 1
    own, other = own_ref[...].astype(F32), other_ref[...].astype(F32)
    second = jnp.where(right, own, other).astype(BF16)
    first = jnp.where(right, other, own).astype(BF16)
    second_ref[...] = second
    whole = dot(first, second)
    whole_ref[...] = whole
    half = half_ref.shape[0]
    half_ref[...] = jnp.where(right, whole[half:], whole[:half])
    width = whole.shape[0]
    row = lax.broadcasted_iota(jnp.int32, (width, width), 0)
    col = lax.broadcasted_iota(jnp.int32, (width, width), 1)
    prefix_ref[...] = jnp.where(right, other, jnp.where(row == col, 1.0, 0.0))


def static_kernel(flags_ref, whole_ref, got_ref, twin_ref, prefix_ref, *outs, more, chain):
    even, right = flags_ref[0] == 1, flags_ref[1] == 1
    half = got_ref.shape[0]
    got, twin = got_ref[...], twin_ref[...]
    other = jnp.concatenate([jnp.where(even, got, twin), jnp.where(even, twin, got)], 0)
    whole = whole_ref[...]
    second3 = split3(jnp.where(right, whole, other))
    first3 = split3(jnp.where(right, other, whole))
    prefix = prefix_ref[...]
    reach_ref, second_ref, prefix_out = outs[:3]
    for j, part in enumerate(split3(prefix)):
        reach_ref[j] = part
    for j, part in enumerate(second3):
        second_ref[j] = part
    if chain:
        whole_out, half_out = outs[3:]
        both = times_split(first3, *second3)
        whole_out[...] = both
        half_out[...] = jnp.where(even, both[:half], both[half:])
    prefix3 = split3(prefix)
    prefix_out[...] = jnp.where(right, times_split(first3, *prefix3), prefix)


def level0_kernel(right_ref, both_ref, got_ref, second_ref, total_ref, carry_ref):
    right = right_ref[0] == 1
    rows = total_ref.shape[0]
    total, got = both_ref[:rows, :], got_ref[:rows, :]
    carry_ref[...] = jnp.where(right, got, 0.0)
    first = split3(jnp.where(right, got, total))
    total_ref[...] = times_exact(first, second_ref[...]) + jnp.where(right, total, got)


def level_kernel(right_ref, total_ref, got_ref, carry_ref, reach_ref, second_ref, total_out, carry_out):
    right = right_ref[0] == 1
    total, got = total_ref[...], got_ref[...]
    first = split3(jnp.where(right, got, total))
    total_out[...] = times_split(first, *(second_ref[j] for j in range(3))) + jnp.where(right, total, got)
    step = times_split(first, *(reach_ref[j] for j in range(3)))
    carry_out[...] = carry_ref[...] + jnp.where(right, step, 0.0)


def tips_kernel(
    flags_ref, got_ref, carry_ref, reach_ref, both_ref, near_ref, far_ref, local_ref, x_ref, u_ref, l_ref,
    before_ref, after_ref, chain_ref, top_out, previous_out, near_out, far_out,
):
    even, right = flags_ref[0] == 1, flags_ref[1] == 1
    rows, width = got_ref.shape
    carry = carry_ref[...]
    if reach_ref is not None:
        step = times_split(split3(got_ref[...]), *(reach_ref[j] for j in range(3)))
        carry = carry + jnp.where(right, step, 0.0)
    own_top = local_ref[:, :width]
    own_bottom = local_ref[:, -width:]
    next_top = jnp.where(even, near_ref[rows:, :], far_ref[...])
    previous = carry - times_exact(split3(own_top), before_ref[...])
    offset = own_bottom - times_exact(split3(next_top), u_ref[:, -width:])
    bottom = offset + times_exact(split3(previous), chain_ref[...])
    top = (next_top - times_exact(split3(bottom), after_ref[...])).astype(BF16)
    previous = previous.astype(BF16)
    top_out[...] = top
    previous_out[...] = previous

    def updated(columns):
        change = local_ref[:, columns] - dot(top, u_ref[:, columns]) - dot(previous, l_ref[:, columns])
        return x_ref[:, columns] + change

    size = x_ref.shape[1]
    first = updated(slice(0, width))
    final = updated(slice(size - width, size))
    near_out[...] = jnp.where(even, final, first)
    far_out[...] = jnp.where(even, first, final)


def update_kernel(top_ref, previous_ref, local_ref, x_ref, u_ref, l_ref, b_ref, d3_ref, s3_ref, p3_ref, x_out, acc_ref):
    change = local_ref[...] - dot(top_ref[...], u_ref[...]) - dot(previous_ref[...], l_ref[...])
    x_out[...] = x_ref[...] + change
    local_part(b_ref, x_out, d3_ref, s3_ref, p3_ref, acc_ref)


def body(
    right_sides,
    initial,
    diag_blocks,
    sub_blocks,
    super_blocks,
    local_inverse,
    upper_spikes,
    lower_spikes,
):
    width = diag_blocks.shape[1]
    rows, size = right_sides.shape
    count = lax.axis_size(AXIS)
    here = lax.axis_index(AXIS)
    levels = (count - 1).bit_length()
    bits = [((here >> level) & 1).astype(jnp.int32) for level in range(levels)]
    even = (1 - bits[0])[None]
    rights = [bit[None] for bit in bits]
    tip = ((rows, width), F32)
    square = ((width, width), F32)
    low_square = ((width, width), BF16)
    triple = ((3, width, width), BF16)
    half = ((width // 2, width), F32)
    wide = ((rows, size), F32)
    big = ((3, size, width), BF16)

    x_near, x_far, s_near, s_far, chain = kernel_call(
        payload_kernel, [tip, tip, low_square, low_square, low_square], even, initial, upper_spikes, lower_spikes
    )
    near, far = exchange(x_near, 1), across(x_far)
    other = exchange(chain, 1)
    s_near, s_far = exchange(s_near, 1), across(s_far)
    acc, d3, s3, p3 = kernel_call(
        first_local_kernel, [wide, big, big, big], right_sides, initial, diag_blocks, sub_blocks, super_blocks, scalars=0
    )
    before, after, mix = kernel_call(mix_kernel, [low_square, low_square, triple], even, s_near, s_far, chain)

    whole, piece, second, prefix = kernel_call(
        start_static_kernel, [square, half, low_square, square], rights[0], chain, other
    )
    mats = [(None, second)]
    for level in range(1, levels - 1):
        got = exchange(piece, 1 << level)
        twin = exchange(got, 1)
        flags = jnp.concatenate([even, rights[level]])
        chained = level < levels - 2
        outs = [triple, triple, square] + ([square, half] if chained else [])
        reach, second, prefix, *rest = kernel_call(
            functools.partial(static_kernel, more=True, chain=chained), outs, flags, whole, got, twin, prefix
        )
        if chained:
            whole, piece = rest
        mats.append((reach, second))
    last_reach = kernel_call(split_kernel, [triple], prefix, scalars=0)[0]

    solution = initial
    norms = []
    for turn in range(ITERS):
        both, local, norm = kernel_call(
            solve_kernel, [((2 * rows, width), F32), wide, ((rows, 1), F32)],
            even, acc, near, far, s3, p3, local_inverse, mix,
        )
        norms.append(norm)
        swapped = exchange(both, 1)
        far_top = across(both[rows:])
        total, carry = kernel_call(level0_kernel, [tip, tip], rights[0], both, swapped, mats[0][1])
        for level in range(1, levels - 1):
            got = exchange(total, 1 << level)
            reach, second = mats[level]
            total, carry = kernel_call(level_kernel, [tip, tip], rights[level], total, got, carry, reach, second)
        got = exchange(total, 1 << (levels - 1))
        top, previous, near, far = kernel_call(
            tips_kernel, [tip[:1] + (BF16,), tip[:1] + (BF16,), tip, tip], jnp.concatenate([even, rights[-1]]),
            got, carry, last_reach, both, swapped, far_top, local, solution, upper_spikes, lower_spikes, before, after, chain,
        )
        near, far = exchange(near, 1), across(far)
        solution, acc = kernel_call(
            update_kernel, [wide, wide], top, previous, local, solution, upper_spikes, lower_spikes, right_sides, d3, s3, p3,
            scalars=0,
        )
    norms.append(kernel_call(norm_kernel, [((rows, 1), F32)], even, acc, near, far, s3, p3)[0])
    mine = jnp.concatenate(norms, 1).T.reshape(1, -1)
    gathered = lax.all_to_all(jnp.broadcast_to(mine, (count, mine.shape[1])), AXIS, 0, 0)
    totals = jnp.sum(gathered, axis=0).reshape(ITERS + 1, rows)
    return (solution, jnp.sqrt(totals / (size * count)))


def split_kernel(values_ref, out_ref):
    for j, part in enumerate(split3(values_ref[...])):
        out_ref[j] = part


def solution(mesh):
    return jax.shard_map(
        body,
        mesh=mesh,
        in_specs=(
            P(None, AXIS),
            P(None, AXIS),
            P(AXIS, None),
            P(AXIS, None),
            P(AXIS, None),
            P(AXIS, None),
            P(None, AXIS),
            P(None, AXIS),
        ),
        out_specs=(P(None, AXIS), P()),
        check_vma=False,
    )
```

```python
import functools
import math

import jax
import jax.numpy as jnp
from jax import lax
from jax.experimental import pallas as pl
from jax.experimental.pallas import tpu as pltpu
from jax.sharding import PartitionSpec as P


ITERS = 2
AXIS = "rows"
F32 = jnp.float32
BF16 = jnp.bfloat16


def exchange(values, distance):
    count = lax.axis_size(AXIS)
    return lax.ppermute(values, AXIS, [(i, i ^ distance) for i in range(count)])


def across(values):
    count = lax.axis_size(AXIS)
    pairs = [(i, i + 1) for i in range(1, count - 1, 2)]
    return lax.ppermute(values, AXIS, pairs + [(b, a) for a, b in pairs])


def kernel_call(kernel, outs, *args, micros=0.3):
    specs = [
        pl.BlockSpec(memory_space=pltpu.HBM if isinstance(a, tuple) else pltpu.VMEM) for a in args
    ]
    held = sum(math.prod(shape) * jnp.dtype(dtype).itemsize for shape, dtype in outs)
    return pl.pallas_call(
        kernel,
        in_specs=specs,
        out_specs=[pl.BlockSpec(memory_space=pltpu.VMEM)] * len(outs),
        out_shape=[pltpu.VMEM(shape, dtype) for shape, dtype in outs],
        scratch_shapes=[],
        cost_estimate=pl.CostEstimate(flops=int(micros * 1e8), transcendentals=0, bytes_accessed=held),
        compiler_params=pltpu.CompilerParams(vmem_limit_bytes=16 * 2**20),
    )(*(pltpu.with_memory_space_constraint(a[0], pltpu.HBM) if isinstance(a, tuple) else a for a in args))


def is_even():
    return lax.axis_index(AXIS) % 2 == 0


def on_right(level):
    return (lax.axis_index(AXIS) >> level) % 2 == 1


def split3(values):
    high = values.astype(BF16)
    rest = values - high.astype(F32)
    mid = rest.astype(BF16)
    low = (rest - mid.astype(F32)).astype(BF16)
    return high, mid, low


def dot(left, right):
    return jnp.dot(left, right, preferred_element_type=F32)


def fold(product, count):
    rows = product.shape[0] // count
    total = product[(count - 1) * rows :]
    for i in range(count - 2, -1, -1):
        total = total + product[i * rows : (i + 1) * rows]
    return total


def times_exact(parts, right):
    return fold(dot(jnp.concatenate(parts, 0), right), 3)


def times_split(parts, high, mid, low):
    small = dot(parts[0], low) + fold(dot(jnp.concatenate(parts[:2], 0), mid), 2)
    return fold(dot(jnp.concatenate(parts, 0), high), 3) + small


def gather_copies(pairs, sems):
    copies = [pltpu.make_async_copy(a, b, sems.at[i]) for i, (a, b) in enumerate(pairs)]
    for copy in copies:
        copy.start()
    return copies


def payload_kernel(x_hbm, u_hbm, l_hbm, xn_ref, xf_ref, sn_ref, sf_ref, chain_ref):
    even = is_even()
    width = xn_ref.shape[1]
    last = x_hbm.shape[1] - width

    def work(first, final, up, low, bottom, sems):
        head, tail = pl.ds(0, width), pl.ds(last, width)
        copies = gather_copies(
            [
                (x_hbm.at[:, head], first),
                (x_hbm.at[:, tail], final),
                (l_hbm.at[:, tail], bottom),
                (u_hbm.at[:, tail], up),
                (l_hbm.at[:, head], low),
            ],
            sems,
        )
        for copy in copies:
            copy.wait()
        xn_ref[...] = jnp.where(even, final[...], first[...])
        xf_ref[...] = jnp.where(even, first[...], final[...])
        chain_ref[...] = -bottom[...]
        low_tip, up_tip = low[...].astype(F32), up[...].astype(F32)
        sn_ref[...] = jnp.where(even, up_tip, low_tip).astype(BF16)
        sf_ref[...] = jnp.where(even, low_tip, up_tip).astype(BF16)

    vec = pltpu.VMEM(xn_ref.shape, F32)
    mat = pltpu.VMEM(sn_ref.shape, BF16)
    pl.run_scoped(work, vec, vec, mat, mat, mat, pltpu.SemaphoreType.DMA((5,)))


def split_store(ref, rows, values):
    for j, part in enumerate(split3(values)):
        ref[j, rows, :] = part


def first_local_kernel(b_hbm, x_hbm, d_hbm, s_hbm, p_hbm, z_hbm, u_hbm, l_hbm, acc_ref, b_ref, x_ref, d3_ref, s3_ref, p3_ref, z_ref, u_ref, l_ref):
    width = d_hbm.shape[1]

    def work(d_ref, s_ref, p_ref, sems):
        copies = gather_copies(
            [(x_hbm, x_ref), (d_hbm, d_ref), (s_hbm, s_ref), (p_hbm, p_ref), (b_hbm, b_ref), (z_hbm, z_ref), (u_hbm, u_ref), (l_hbm, l_ref)],
            sems,
        )
        for copy in copies[:2]:
            copy.wait()
        for source, target, copy in ((d_ref, d3_ref, 2), (s_ref, s3_ref, 3), (p_ref, p3_ref, 4)):
            for k in range(d_ref.shape[0] // width):
                split_store(target, pl.ds(k * width, width), source[k * width : (k + 1) * width, :])
            copies[copy].wait()
        local_part(b_ref, x_ref, d3_ref, s3_ref, p3_ref, acc_ref)
        for copy in copies[5:]:
            copy.wait()

    mat = pltpu.VMEM(d_hbm.shape, F32)
    pl.run_scoped(work, mat, mat, mat, pltpu.SemaphoreType.DMA((8,)))


def local_part(b_ref, x_ref, d3_ref, s3_ref, p3_ref, acc_ref):
    width = d3_ref.shape[2]
    last = d3_ref.shape[1] // width - 1
    x = [split3(x_ref[:, k * width : (k + 1) * width]) for k in range(last + 1)]
    for k in range(last + 1):
        rows = pl.ds(k * width, width)
        part = times_split(x[k], *(d3_ref[j, rows, :] for j in range(3)))
        if k > 0:
            part = part + times_split(x[k - 1], *(s3_ref[j, rows, :] for j in range(3)))
        if k < last:
            part = part + times_split(x[k + 1], *(p3_ref[j, rows, :] for j in range(3)))
        acc_ref[:, k * width : (k + 1) * width] = b_ref[:, k * width : (k + 1) * width] - part


def close_residual(acc_ref, near_ref, far_ref, s3_ref, p3_ref):
    even = is_even()
    width = s3_ref.shape[2]
    last = s3_ref.shape[1] - width
    near, far = near_ref[...], far_ref[...]
    before = split3(jnp.where(even, far, near))
    after = split3(jnp.where(even, near, far))
    first = acc_ref[:, :width] - times_split(before, *(s3_ref[j, :width, :] for j in range(3)))
    final = acc_ref[:, last:] - times_split(after, *(p3_ref[j, last:, :] for j in range(3)))
    return first, acc_ref[:, width:last], final


def squares(parts, turn, lanes):
    total = sum(jnp.sum(p * p, axis=1, keepdims=True) for p in parts)
    rows = total.shape[0]
    row = lax.broadcasted_iota(jnp.int32, (rows, lanes), 0)
    lane = lax.broadcasted_iota(jnp.int32, (rows, lanes), 1)
    return jnp.sum(jnp.where(lane == row + turn * rows, total, 0.0), axis=0, keepdims=True)


def solve_kernel(acc_ref, near_ref, far_ref, s3_ref, p3_ref, z_ref, mix_ref, norm_in, both_ref, top_ref, local_ref, norm_ref, *, turn):
    parts = close_residual(acc_ref, near_ref, far_ref, s3_ref, p3_ref)
    width = s3_ref.shape[2]
    rows = acc_ref.shape[0]
    rounded = jnp.concatenate([p.astype(BF16) for p in parts], 1)
    local = dot(rounded, z_ref[...])
    local_ref[...] = local
    own_top = local[:, :width]
    mixed = times_split(split3(own_top), *(mix_ref[j] for j in range(3)))
    both_ref[:rows, :] = local[:, -width:] - mixed
    both_ref[rows:, :] = own_top
    top_ref[...] = own_top
    norm = squares(parts, turn, norm_ref.shape[1])
    norm_ref[...] = norm if norm_in is None else norm_in[...] + norm


def norm_kernel(acc_ref, near_ref, far_ref, s3_ref, p3_ref, norm_in, norm_ref, *, turn):
    norm = squares(close_residual(acc_ref, near_ref, far_ref, s3_ref, p3_ref), turn, norm_ref.shape[1])
    norm_ref[...] = jnp.broadcast_to(norm_in[...] + norm, norm_ref.shape)


def mix_kernel(near_ref, far_ref, chain_ref, before_ref, after_ref, mix_ref):
    even = is_even()
    near, far = near_ref[...].astype(F32), far_ref[...].astype(F32)
    before = jnp.where(even, far, near).astype(BF16)
    before_ref[...] = before
    after_ref[...] = jnp.where(even, near, far).astype(BF16)
    for j, part in enumerate(split3(dot(before, chain_ref[...]))):
        mix_ref[j] = part


def start_static_kernel(own_ref, other_ref, second_ref, prefix_ref, whole_ref=None, half_ref=None):
    right = on_right(0)
    own, other = own_ref[...].astype(F32), other_ref[...].astype(F32)
    second = jnp.where(right, own, other).astype(BF16)
    first = jnp.where(right, other, own).astype(BF16)
    second_ref[...] = second
    width = own.shape[0]
    row = lax.broadcasted_iota(jnp.int32, (width, width), 0)
    col = lax.broadcasted_iota(jnp.int32, (width, width), 1)
    prefix = jnp.where(right, other, jnp.where(row == col, 1.0, 0.0))
    for j, part in enumerate(split3(prefix)):
        prefix_ref[j] = part
    if whole_ref is not None:
        whole = dot(first, second)
        half = half_ref.shape[0]
        half_ref[...] = jnp.where(right, whole[half:], whole[:half])
        whole_ref[...] = whole


def static_kernel(whole_ref, got_ref, twin_ref, prefix_ref, second_ref, prefix_out, whole_out=None, half_out=None, *, level):
    even, right = is_even(), on_right(level)
    half = got_ref.shape[0]
    got, twin = got_ref[...], twin_ref[...]
    other = jnp.concatenate([jnp.where(even, got, twin), jnp.where(even, twin, got)], 0)
    whole = whole_ref[...]
    second3 = split3(jnp.where(right, whole, other))
    first3 = split3(jnp.where(right, other, whole))
    for j, part in enumerate(second3):
        second_ref[j] = part
    if whole_out is not None:
        both = times_split(first3, *second3)
        whole_out[...] = both
        half_out[...] = jnp.where(even, both[:half], both[half:])
    prefix = [prefix_ref[j] for j in range(3)]
    for j, part in enumerate(split3(times_split(first3, *prefix))):
        prefix_out[j] = jnp.where(right, part.astype(F32), prefix[j].astype(F32)).astype(BF16)


def level0_kernel(both_ref, got_ref, second_ref, total_ref, carry_ref):
    right = on_right(0)
    rows = total_ref.shape[0]
    total, got = both_ref[:rows, :], got_ref[:rows, :]
    carry_ref[...] = jnp.where(right, got, 0.0)
    first = split3(jnp.where(right, got, total))
    total_ref[...] = times_exact(first, second_ref[...]) + jnp.where(right, total, got)


def level_kernel(total_ref, got_ref, carry_ref, reach_ref, second_ref, total_out, carry_out, *, level):
    right = on_right(level)
    total, got = total_ref[...], got_ref[...]
    first = split3(jnp.where(right, got, total))
    total_out[...] = times_split(first, *(second_ref[j] for j in range(3))) + jnp.where(right, total, got)
    step = times_split(first, *(reach_ref[j] for j in range(3)))
    carry_out[...] = carry_ref[...] + jnp.where(right, step, 0.0)


def tips_kernel(
    got_ref, carry_ref, reach_ref, near_ref, far_ref, local_ref, x_ref, u_ref, l_ref,
    before_ref, after_ref, chain_ref, top_out, previous_out, near_out, far_out, *, level
):
    even, right = is_even(), on_right(level)
    rows, width = got_ref.shape
    step = times_split(split3(got_ref[...]), *(reach_ref[j] for j in range(3)))
    carry = carry_ref[...] + jnp.where(right, step, 0.0)
    own_top = local_ref[:, :width]
    own_bottom = local_ref[:, -width:]
    next_top = jnp.where(even, near_ref[rows:, :], far_ref[...])
    offset = own_bottom - times_exact(split3(next_top), u_ref[:, -width:])
    previous = carry - times_exact(split3(own_top), before_ref[...])
    bottom = offset + times_exact(split3(previous), chain_ref[...])
    top = (next_top - times_exact(split3(bottom), after_ref[...])).astype(BF16)
    previous = previous.astype(BF16)
    top_out[...] = top
    previous_out[...] = previous

    def updated(columns):
        change = local_ref[:, columns] - dot(top, u_ref[:, columns]) - dot(previous, l_ref[:, columns])
        return x_ref[:, columns] + change

    size = x_ref.shape[1]
    first = updated(slice(0, width))
    final = updated(slice(size - width, size))
    near_out[...] = jnp.where(even, final, first)
    far_out[...] = jnp.where(even, first, final)


def update_kernel(top_ref, previous_ref, local_ref, x_ref, u_ref, l_ref, b_ref, d3_ref, s3_ref, p3_ref, x_out, acc_ref):
    change = local_ref[...] - dot(top_ref[...], u_ref[...]) - dot(previous_ref[...], l_ref[...])
    x_out[...] = x_ref[...] + change
    local_part(b_ref, x_out, d3_ref, s3_ref, p3_ref, acc_ref)


def finish_kernel(gathered_ref, out_ref, *, total):
    sums = jnp.sqrt(jnp.sum(gathered_ref[...], axis=0, keepdims=True) / total)
    rows = out_ref.shape[1]
    for turn in range(out_ref.shape[0]):
        out_ref[pl.ds(turn, 1), :] = sums[:, turn * rows : (turn + 1) * rows]


def body(
    right_sides,
    initial,
    diag_blocks,
    sub_blocks,
    super_blocks,
    local_inverse,
    upper_spikes,
    lower_spikes,
):
    width = diag_blocks.shape[1]
    rows, size = right_sides.shape
    count = lax.axis_size(AXIS)
    levels = (count - 1).bit_length()
    tip = ((rows, width), F32)
    low_tip = ((rows, width), BF16)
    square = ((width, width), F32)
    low_square = ((width, width), BF16)
    triple = ((3, width, width), BF16)
    half = ((width // 2, width), F32)
    wide = ((rows, size), F32)
    big = ((3, size, width), BF16)
    lanes = -(-rows * (ITERS + 1) // 128) * 128
    norm_row = ((1, lanes), F32)

    x_near, x_far, s_near, s_far, chain = kernel_call(
        payload_kernel, [tip, tip, low_square, low_square, low_square], (initial,), (upper_spikes,), (lower_spikes,)
    )
    near = exchange(x_near, 1)
    far = across(x_far)
    other = exchange(chain, 1)
    s_near = exchange(s_near, 1)
    s_far = across(s_far)
    acc, right_sides, solution, d3, s3, p3, local_inverse, upper_spikes, lower_spikes = kernel_call(
        first_local_kernel,
        [wide, wide, wide, big, big, big, (local_inverse.shape, BF16), (upper_spikes.shape, BF16), (lower_spikes.shape, BF16)],
        *((a,) for a in (right_sides, initial, diag_blocks, sub_blocks, super_blocks, local_inverse, upper_spikes, lower_spikes)),
        micros=3,
    )
    before, after, mix = kernel_call(mix_kernel, [low_square, low_square, triple], s_near, s_far, chain)

    outs = [square, half]
    second, prefix, *rest = kernel_call(start_static_kernel, [low_square, triple] + outs * (levels > 2), chain, other)
    mats = [(None, second)]
    for level in range(1, levels - 1):
        whole, piece = rest
        got = exchange(piece, 1 << level)
        twin = exchange(got, 1)
        reach = prefix
        second, prefix, *rest = kernel_call(
            functools.partial(static_kernel, level=level),
            [triple, triple] + outs * (level < levels - 2), whole, got, twin, prefix, micros=1,
        )
        mats.append((reach, second))

    norm = None
    for turn in range(ITERS):
        args = [acc, near, far, s3, p3, local_inverse, mix]
        solve = functools.partial(solve_kernel, turn=turn)
        if norm is None:
            solve = functools.partial(lambda *refs, turn: solve_kernel(*refs[:7], None, *refs[7:], turn=turn), turn=turn)
        else:
            args.append(norm)
        both, own_top, local, norm = kernel_call(
            solve, [((2 * rows, width), F32), tip, wide, norm_row], *args, micros=0.8
        )
        swapped = exchange(both, 1)
        far_top = across(own_top)
        total, carry = kernel_call(level0_kernel, [tip, tip], both, swapped, mats[0][1])
        for level in range(1, levels - 1):
            got = exchange(total, 1 << level)
            reach, second = mats[level]
            total, carry = kernel_call(
                functools.partial(level_kernel, level=level), [tip, tip], total, got, carry, reach, second
            )
        got = exchange(total, 1 << (levels - 1))
        top, previous, near, far = kernel_call(
            functools.partial(tips_kernel, level=levels - 1), [low_tip, low_tip, tip, tip],
            got, carry, prefix, swapped, far_top, local, solution, upper_spikes, lower_spikes, before, after, chain, micros=1,
        )
        near = exchange(near, 1)
        far = across(far)
        solution, acc = kernel_call(
            update_kernel, [wide, wide],
            top, previous, local, solution, upper_spikes, lower_spikes, right_sides, d3, s3, p3, micros=1,
        )
    mine = kernel_call(
        functools.partial(norm_kernel, turn=ITERS), [((count, lanes), F32)], acc, near, far, s3, p3, norm
    )[0]
    gathered = lax.all_to_all(mine, AXIS, 0, 0, tiled=True)
    norms = pl.pallas_call(
        functools.partial(finish_kernel, total=size * count), out_shape=jax.ShapeDtypeStruct((ITERS + 1, rows), F32),
        compiler_params=pltpu.CompilerParams(vmem_limit_bytes=16 * 2**20),
    )(gathered)
    return solution, norms


def solution(mesh):
    return jax.shard_map(
        body,
        mesh=mesh,
        in_specs=(
            P(None, AXIS),
            P(None, AXIS),
            P(AXIS, None),
            P(AXIS, None),
            P(AXIS, None),
            P(AXIS, None),
            P(None, AXIS),
            P(None, AXIS),
        ),
        out_specs=(P(None, AXIS), P()),
        check_vma=False,
    )
```

```python
import functools
import math

import jax
import jax.numpy as jnp
from jax import lax
from jax.experimental import pallas as pl
from jax.experimental.pallas import tpu as pltpu
from jax.sharding import PartitionSpec as P


ITERS = 2
AXIS = "rows"
F32 = jnp.float32
BF16 = jnp.bfloat16


def exchange(values, distance):
    count = lax.axis_size(AXIS)
    return lax.ppermute(values, AXIS, [(i, i ^ distance) for i in range(count)])


def across(values):
    count = lax.axis_size(AXIS)
    pairs = [(i, i + 1) for i in range(1, count - 1, 2)]
    return lax.ppermute(values, AXIS, pairs + [(b, a) for a, b in pairs])


def kernel_call(kernel, outs, *args, micros=0.3):
    specs = [
        pl.BlockSpec(memory_space=pltpu.HBM if isinstance(a, tuple) else pltpu.VMEM) for a in args
    ]
    held = sum(math.prod(shape) * jnp.dtype(dtype).itemsize for shape, dtype in outs)
    return pl.pallas_call(
        kernel,
        in_specs=specs,
        out_specs=[pl.BlockSpec(memory_space=pltpu.VMEM)] * len(outs),
        out_shape=[pltpu.VMEM(shape, dtype) for shape, dtype in outs],
        scratch_shapes=[],
        cost_estimate=pl.CostEstimate(flops=int(micros * 1e8), transcendentals=0, bytes_accessed=held),
        compiler_params=pltpu.CompilerParams(vmem_limit_bytes=16 * 2**20),
    )(*(pltpu.with_memory_space_constraint(a[0], pltpu.HBM) if isinstance(a, tuple) else a for a in args))


def is_even():
    return lax.axis_index(AXIS) % 2 == 0


def on_right(level):
    return (lax.axis_index(AXIS) >> level) % 2 == 1


def split3(values):
    high = values.astype(BF16)
    rest = values - high.astype(F32)
    mid = rest.astype(BF16)
    low = (rest - mid.astype(F32)).astype(BF16)
    return high, mid, low


def dot(left, right):
    return jnp.dot(left, right, preferred_element_type=F32)


def fold(product, count):
    rows = product.shape[0] // count
    total = product[(count - 1) * rows :]
    for i in range(count - 2, -1, -1):
        total = total + product[i * rows : (i + 1) * rows]
    return total


def times_exact(parts, right):
    return fold(dot(jnp.concatenate(parts, 0), right), 3)


def times_split(parts, high, mid, low):
    small = dot(parts[0], low) + fold(dot(jnp.concatenate(parts[:2], 0), mid), 2)
    return fold(dot(jnp.concatenate(parts, 0), high), 3) + small


def gather_copies(pairs, sems):
    copies = [pltpu.make_async_copy(a, b, sems.at[i]) for i, (a, b) in enumerate(pairs)]
    for copy in copies:
        copy.start()
    return copies


def payload_kernel(x_hbm, u_hbm, l_hbm, near_ref, far_ref, chain_ref):
    even = is_even()
    width = chain_ref.shape[0]
    rows = x_hbm.shape[0]
    last = x_hbm.shape[1] - width

    def work(first, final, up, low, bottom, sems):
        head, tail = pl.ds(0, width), pl.ds(last, width)
        copies = gather_copies(
            [
                (x_hbm.at[:, head], first),
                (x_hbm.at[:, tail], final),
                (l_hbm.at[:, tail], bottom),
                (u_hbm.at[:, tail], up),
                (l_hbm.at[:, head], low),
            ],
            sems,
        )
        for copy in copies:
            copy.wait()
        for ref, here, there in ((near_ref, final, first), (far_ref, first, final)):
            for j, part in enumerate(split3(jnp.where(even, here[...], there[...]))):
                ref[pl.ds(j * rows, rows), :] = part
        chain = -bottom[...]
        chain_ref[...] = chain
        low_tip, up_tip = low[...].astype(F32), up[...].astype(F32)
        near_ref[pl.ds(3 * rows, width), :] = jnp.where(even, up_tip, low_tip).astype(BF16)
        far_ref[pl.ds(3 * rows, width), :] = jnp.where(even, low_tip, up_tip).astype(BF16)
        near_ref[pl.ds(3 * rows + width, width), :] = chain

    vec = pltpu.VMEM((rows, width), F32)
    mat = pltpu.VMEM(chain_ref.shape, BF16)
    pl.run_scoped(work, vec, vec, mat, mat, mat, pltpu.SemaphoreType.DMA((5,)))


def split_store(ref, rows, values):
    for j, part in enumerate(split3(values)):
        ref[j, rows, :] = part


def first_local_kernel(b_hbm, x_hbm, d_hbm, s_hbm, p_hbm, z_hbm, u_hbm, l_hbm, acc_ref, b_ref, x_ref, d3_ref, s3_ref, p3_ref, z_ref, u_ref, l_ref):
    width = d_hbm.shape[1]

    def work(d_ref, s_ref, p_ref, sems):
        copies = gather_copies(
            [(x_hbm, x_ref), (d_hbm, d_ref), (s_hbm, s_ref), (p_hbm, p_ref), (b_hbm, b_ref), (z_hbm, z_ref), (u_hbm, u_ref), (l_hbm, l_ref)],
            sems,
        )
        for copy in copies[:2]:
            copy.wait()
        for source, target, copy in ((d_ref, d3_ref, 2), (s_ref, s3_ref, 3), (p_ref, p3_ref, 4)):
            for k in range(d_ref.shape[0] // width):
                split_store(target, pl.ds(k * width, width), source[k * width : (k + 1) * width, :])
            copies[copy].wait()
        local_part(b_ref, x_ref, d3_ref, s3_ref, p3_ref, acc_ref)
        for copy in copies[5:]:
            copy.wait()

    mat = pltpu.VMEM(d_hbm.shape, F32)
    pl.run_scoped(work, mat, mat, mat, pltpu.SemaphoreType.DMA((8,)))


def local_part(b_ref, x_ref, d3_ref, s3_ref, p3_ref, acc_ref):
    width = d3_ref.shape[2]
    last = d3_ref.shape[1] // width - 1
    x = [split3(x_ref[:, k * width : (k + 1) * width]) for k in range(last + 1)]
    for k in range(last + 1):
        rows = pl.ds(k * width, width)
        part = times_split(x[k], *(d3_ref[j, rows, :] for j in range(3)))
        if k > 0:
            part = part + times_split(x[k - 1], *(s3_ref[j, rows, :] for j in range(3)))
        if k < last:
            part = part + times_split(x[k + 1], *(p3_ref[j, rows, :] for j in range(3)))
        acc_ref[:, k * width : (k + 1) * width] = b_ref[:, k * width : (k + 1) * width] - part


def choose(condition, left, right):
    return jnp.where(condition, left.astype(F32), right.astype(F32)).astype(left.dtype)


def sides_of(near_ref, far_ref, rows):
    even = is_even()
    if near_ref.dtype == F32:
        near, far = near_ref[...], far_ref[...]
        return split3(jnp.where(even, far, near)), split3(jnp.where(even, near, far))
    near = [near_ref[pl.ds(j * rows, rows), :] for j in range(3)]
    far = [far_ref[pl.ds(j * rows, rows), :] for j in range(3)]
    before = [choose(even, f, n) for n, f in zip(near, far)]
    after = [choose(even, n, f) for n, f in zip(near, far)]
    return before, after


def close_residual(acc_ref, near_ref, far_ref, s3_ref, p3_ref):
    width = s3_ref.shape[2]
    last = s3_ref.shape[1] - width
    before, after = sides_of(near_ref, far_ref, acc_ref.shape[0])
    first = acc_ref[:, :width] - times_split(before, *(s3_ref[j, :width, :] for j in range(3)))
    final = acc_ref[:, last:] - times_split(after, *(p3_ref[j, last:, :] for j in range(3)))
    return first, acc_ref[:, width:last], final


def squares(parts):
    total = None
    for part in parts:
        for i in range(0, part.shape[1], 128):
            piece = part[:, i : i + 128]
            total = piece * piece if total is None else total + piece * piece
    return total


def lane_row(total, turn, lanes):
    total = jnp.sum(total, axis=1, keepdims=True)
    rows = total.shape[0]
    row = lax.broadcasted_iota(jnp.int32, (rows, lanes), 0)
    lane = lax.broadcasted_iota(jnp.int32, (rows, lanes), 1)
    return jnp.sum(jnp.where(lane == row + turn * rows, total, 0.0), axis=0, keepdims=True)


def solve_kernel(acc_ref, near_ref, far_ref, s3_ref, p3_ref, z_ref, mix_ref, both_ref, top_ref, local_ref, norm_ref):
    parts = close_residual(acc_ref, near_ref, far_ref, s3_ref, p3_ref)
    width = s3_ref.shape[2]
    rows = acc_ref.shape[0]
    rounded = jnp.concatenate([p.astype(BF16) for p in parts], 1)
    local = dot(rounded, z_ref[...])
    local_ref[...] = local
    own_top = local[:, :width]
    mixed = times_split(split3(own_top), *(mix_ref[j] for j in range(3)))
    both_ref[:rows, :] = local[:, -width:] - mixed
    both_ref[rows:, :] = own_top
    top_ref[...] = own_top
    norm_ref[...] = squares(parts)


def norm_kernel(acc_ref, near_ref, far_ref, s3_ref, p3_ref, middle_ref, rest_ref, norm_ref, *, turn):
    first, _, final = close_residual(acc_ref, near_ref, far_ref, s3_ref, p3_ref)
    row = rest_ref[...] + lane_row(middle_ref[...] + squares((first, final)), turn, norm_ref.shape[1])
    norm_ref[...] = jnp.broadcast_to(row, norm_ref.shape)


def mix_kernel(near_ref, far_ref, chain_ref, before_ref, after_ref, mix_ref):
    even = is_even()
    width = chain_ref.shape[0]
    spikes = pl.ds(far_ref.shape[0] - width, width)
    near, far = near_ref[spikes, :], far_ref[spikes, :]
    before = choose(even, far, near)
    before_ref[...] = before
    after_ref[...] = choose(even, near, far)
    for j, part in enumerate(split3(dot(before, chain_ref[...]))):
        mix_ref[j] = part


def start_static_kernel(own_ref, near_ref, second_ref, prefix_ref, whole_ref=None, half_ref=None):
    right = on_right(0)
    width = own_ref.shape[0]
    own = own_ref[...].astype(F32)
    other = near_ref[pl.ds(near_ref.shape[0] - width, width), :].astype(F32)
    second = jnp.where(right, own, other).astype(BF16)
    first = jnp.where(right, other, own).astype(BF16)
    second_ref[...] = second
    row = lax.broadcasted_iota(jnp.int32, (width, width), 0)
    col = lax.broadcasted_iota(jnp.int32, (width, width), 1)
    prefix = jnp.where(right, other, jnp.where(row == col, 1.0, 0.0))
    for j, part in enumerate(split3(prefix)):
        prefix_ref[j] = part
    if whole_ref is not None:
        whole = dot(first, second)
        half = half_ref.shape[0]
        half_ref[...] = jnp.where(right, whole[half:], whole[:half])
        whole_ref[...] = whole


def static_kernel(whole_ref, got_ref, twin_ref, prefix_ref, second_ref, prefix_out, whole_out=None, half_out=None, *, level):
    even, right = is_even(), on_right(level)
    half = got_ref.shape[0]
    got, twin = got_ref[...], twin_ref[...]
    other = jnp.concatenate([jnp.where(even, got, twin), jnp.where(even, twin, got)], 0)
    whole = whole_ref[...]
    second3 = split3(jnp.where(right, whole, other))
    first3 = split3(jnp.where(right, other, whole))
    for j, part in enumerate(second3):
        second_ref[j] = part
    if whole_out is not None:
        both = times_split(first3, *second3)
        whole_out[...] = both
        half_out[...] = jnp.where(even, both[:half], both[half:])
    prefix = [prefix_ref[j] for j in range(3)]
    for j, part in enumerate(split3(times_split(first3, *prefix))):
        prefix_out[j] = jnp.where(right, part.astype(F32), prefix[j].astype(F32)).astype(BF16)


def merged(right, total, got, matrix):
    first = split3(jnp.where(right, got, total))
    product = times_split(first, *matrix) if isinstance(matrix, list) else times_exact(first, matrix)
    return product + jnp.where(right, total, got)


def parts_of(ref):
    return [ref[j] for j in range(3)]


def carry_step(level, values, reach_ref):
    return jnp.where(on_right(level), times_split(split3(values), *parts_of(reach_ref)), 0.0)


def sent_on(level, total, second_ref, carried_ref):
    product = times_split(split3(total), *parts_of(second_ref))
    carried_ref[...] = jnp.where(on_right(level), total, product)


def level0_kernel(both_ref, got_ref, second_ref, total_ref, carry_ref):
    right = on_right(0)
    rows = total_ref.shape[0]
    total, got = both_ref[:rows, :], got_ref[:rows, :]
    carry_ref[...] = jnp.where(right, got, 0.0)
    total_ref[...] = merged(right, total, got, second_ref[...])


def level0_wide_kernel(both_ref, got_ref, second_ref, next_ref, total_ref, carry_ref, carried_ref):
    level0_kernel(both_ref, got_ref, second_ref, total_ref, carry_ref)
    sent_on(1, total_ref[...], next_ref, carried_ref)


def level_kernel(total_ref, got_ref, carry_ref, reach_ref, second_ref, total_out, carry_out, *, level):
    got = got_ref[...]
    total_out[...] = merged(on_right(level), total_ref[...], got, parts_of(second_ref))
    carry_out[...] = carry_ref[...] + carry_step(level, got, reach_ref)


def wide_kernel(
    total_ref, carried_ref, got_ref, low_ref, cross_ref, carry_ref, reach_ref, reach2_ref, second_ref, second2_ref,
    *rest, level
):
    next_ref = rest[0] if len(rest) == 4 else None
    total_out, carry_out = rest[-3:-1] if next_ref is not None else rest
    right, right2 = on_right(level), on_right(level + 1)
    got, low = got_ref[...], low_ref[...] + cross_ref[...]
    carry_out[...] = carry_ref[...] + carry_step(level, got, reach_ref) + carry_step(level + 1, low, reach2_ref)
    passed = times_split(split3(got), *parts_of(second_ref))
    pair = jnp.where(right, passed + total_ref[...], carried_ref[...] + got)
    total = merged(right2, pair, low, parts_of(second2_ref))
    total_out[...] = total
    if next_ref is not None:
        sent_on(level + 2, total, next_ref, rest[-1])


def tips_kernel(*refs, level, wide):
    gots, refs = refs[: 3 if wide else 1], refs[3 if wide else 1 :]
    reaches, refs = refs[: 2 if wide else 1], refs[2 if wide else 1 :]
    carry_ref, near_ref, far_ref, local_ref, x_ref, u_ref, l_ref, before_ref, after_ref, chain_ref = refs[:10]
    top_out, previous_out, near_out, far_out = refs[10:]
    even = is_even()
    rows, width = carry_ref.shape
    carry = carry_ref[...] + carry_step(level, gots[0][...], reaches[0])
    if wide:
        carry = carry + carry_step(level + 1, gots[1][...] + gots[2][...], reaches[1])
    own_top = local_ref[:, :width]
    own_bottom = local_ref[:, -width:]
    next_top = jnp.where(even, near_ref[rows:, :], far_ref[...])
    offset = own_bottom - times_exact(split3(next_top), u_ref[:, -width:])
    previous = carry - times_exact(split3(own_top), before_ref[...])
    bottom = offset + times_exact(split3(previous), chain_ref[...])
    top = (next_top - times_exact(split3(bottom), after_ref[...])).astype(BF16)
    previous = previous.astype(BF16)
    top_out[...] = top
    previous_out[...] = previous

    def updated(columns):
        change = local_ref[:, columns] - dot(top, u_ref[:, columns]) - dot(previous, l_ref[:, columns])
        return x_ref[:, columns] + change

    size = x_ref.shape[1]
    first = updated(slice(0, width))
    final = updated(slice(size - width, size))
    near_out[...] = jnp.where(even, final, first)
    far_out[...] = jnp.where(even, first, final)


def update_kernel(top_ref, previous_ref, local_ref, x_ref, u_ref, l_ref, b_ref, d3_ref, s3_ref, p3_ref, *refs):
    x_out, acc_ref = refs[-2:] if len(refs) == 2 else refs[-4:-2]
    change = local_ref[...] - dot(top_ref[...], u_ref[...]) - dot(previous_ref[...], l_ref[...])
    x_out[...] = x_ref[...] + change
    local_part(b_ref, x_out, d3_ref, s3_ref, p3_ref, acc_ref)
    if len(refs) > 2:
        norms, middle_ref, row_ref = refs[:-4], refs[-2], refs[-1]
        width = d3_ref.shape[2]
        middle_ref[...] = squares((acc_ref[:, width : acc_ref.shape[1] - width],))
        row_ref[...] = sum(lane_row(ref[...], turn, row_ref.shape[1]) for turn, ref in enumerate(norms))


def finish_kernel(gathered_ref, out_ref, *, total):
    sums = jnp.sqrt(jnp.sum(gathered_ref[...], axis=0, keepdims=True) / total)
    rows = out_ref.shape[1]
    for turn in range(out_ref.shape[0]):
        out_ref[pl.ds(turn, 1), :] = sums[:, turn * rows : (turn + 1) * rows]


def body(
    right_sides,
    initial,
    diag_blocks,
    sub_blocks,
    super_blocks,
    local_inverse,
    upper_spikes,
    lower_spikes,
):
    width = diag_blocks.shape[1]
    rows, size = right_sides.shape
    count = lax.axis_size(AXIS)
    levels = (count - 1).bit_length()
    tip = ((rows, width), F32)
    low_tip = ((rows, width), BF16)
    square = ((width, width), F32)
    low_square = ((width, width), BF16)
    triple = ((3, width, width), BF16)
    half = ((width // 2, width), F32)
    wide = ((rows, size), F32)
    big = ((3, size, width), BF16)
    lanes = -(-rows * (ITERS + 1) // 128) * 128

    near_pack, far_pack, chain = kernel_call(
        payload_kernel,
        [((3 * rows + 2 * width, width), BF16), ((3 * rows + width, width), BF16), low_square],
        (initial,), (upper_spikes,), (lower_spikes,),
    )
    near = exchange(near_pack, 1)
    far = across(far_pack)
    acc, right_sides, solution, d3, s3, p3, local_inverse, upper_spikes, lower_spikes = kernel_call(
        first_local_kernel,
        [wide, wide, wide, big, big, big, (local_inverse.shape, BF16), (upper_spikes.shape, BF16), (lower_spikes.shape, BF16)],
        *((a,) for a in (right_sides, initial, diag_blocks, sub_blocks, super_blocks, local_inverse, upper_spikes, lower_spikes)),
        micros=3,
    )
    before, after, mix = kernel_call(mix_kernel, [low_square, low_square, triple], near, far, chain)

    outs = [square, half]
    second, prefix, *rest = kernel_call(start_static_kernel, [low_square, triple] + outs * (levels > 2), chain, near)
    seconds, reaches = [second], [None, prefix]
    for level in range(1, levels - 1):
        whole, piece = rest
        got = exchange(piece, 1 << level)
        twin = exchange(got, 1)
        second, prefix, *rest = kernel_call(
            functools.partial(static_kernel, level=level),
            [triple, triple] + outs * (level < levels - 2), whole, got, twin, prefix, micros=1,
        )
        seconds.append(second)
        reaches.append(prefix)

    norms = []
    for turn in range(ITERS):
        both, own_top, local, norm = kernel_call(
            solve_kernel, [((2 * rows, width), F32), tip, wide, ((rows, 128), F32)],
            acc, near, far, s3, p3, local_inverse, mix, micros=0.8,
        )
        norms.append(norm)
        swapped = exchange(both, 1)
        far_top = across(own_top)
        groups = [(0, 1)]
        while sum(groups[-1]) < levels:
            level = sum(groups[-1])
            groups.append((level, 2 if turn > 0 and level + 2 <= levels else 1))
        carried = None
        for i, (level, size_of) in enumerate(groups[:-1]):
            after_size = groups[i + 1][1]
            outs = [tip, tip] + [tip] * (after_size == 2)
            following = [seconds[level + size_of]] if after_size == 2 else []
            if level == 0:
                kernel = level0_wide_kernel if after_size == 2 else level0_kernel
                total, carry, *more = kernel_call(kernel, outs, both, swapped, seconds[0], *following)
            elif size_of == 1:
                got = exchange(total, 1 << level)
                total, carry, *more = kernel_call(
                    functools.partial(level_kernel, level=level), outs, total, got, carry, reaches[level], seconds[level]
                )
            else:
                step = 1 << level
                got = exchange(total, step)
                low = exchange(carried, 2 * step)
                cross = exchange(carried, 3 * step)
                total, carry, *more = kernel_call(
                    functools.partial(wide_kernel, level=level), outs, total, carried, got, low, cross, carry,
                    reaches[level], reaches[level + 1], seconds[level], seconds[level + 1], *following,
                )
            carried = more[0] if more else None
        level, size_of = groups[-1]
        gots = [exchange(total, 1 << level)]
        if size_of == 2:
            gots.append(exchange(carried, 2 << level))
            gots.append(exchange(carried, 3 << level))
        top, previous, near, far = kernel_call(
            functools.partial(tips_kernel, level=level, wide=size_of == 2), [low_tip, low_tip, tip, tip],
            *gots, *reaches[level : level + size_of], carry, swapped, far_top, local, solution, upper_spikes, lower_spikes,
            before, after, chain, micros=1,
        )
        near = exchange(near, 1)
        far = across(far)
        final = turn == ITERS - 1
        solution, acc, *sums = kernel_call(
            update_kernel, [wide, wide] + [((rows, 128), F32), ((1, lanes), F32)] * final,
            top, previous, local, solution, upper_spikes, lower_spikes, right_sides, d3, s3, p3, *(norms if final else ()),
            micros=1,
        )
    mine = kernel_call(
        functools.partial(norm_kernel, turn=ITERS), [((count, lanes), F32)], acc, near, far, s3, p3, *sums
    )[0]
    gathered = lax.all_to_all(mine, AXIS, 0, 0, tiled=True)
    result = pl.pallas_call(
        functools.partial(finish_kernel, total=size * count), out_shape=jax.ShapeDtypeStruct((ITERS + 1, rows), F32),
        compiler_params=pltpu.CompilerParams(vmem_limit_bytes=16 * 2**20),
    )(gathered)
    return solution, result


def solution(mesh):
    return jax.shard_map(
        body,
        mesh=mesh,
        in_specs=(
            P(None, AXIS),
            P(None, AXIS),
            P(AXIS, None),
            P(AXIS, None),
            P(AXIS, None),
            P(AXIS, None),
            P(None, AXIS),
            P(None, AXIS),
        ),
        out_specs=(P(None, AXIS), P()),
        check_vma=False,
    )
```

```python
import functools
import math

import jax
import jax.numpy as jnp
from jax import lax
from jax.experimental import pallas as pl
from jax.experimental.pallas import tpu as pltpu
from jax.sharding import PartitionSpec as P


ITERS = 2
AXIS = "rows"
F32 = jnp.float32
BF16 = jnp.bfloat16


def exchange(values, distance):
    count = lax.axis_size(AXIS)
    return lax.ppermute(values, AXIS, [(i, i ^ distance) for i in range(count)])


def across(values):
    count = lax.axis_size(AXIS)
    pairs = [(i, i + 1) for i in range(1, count - 1, 2)]
    return lax.ppermute(values, AXIS, pairs + [(b, a) for a, b in pairs])


def kernel_call(kernel, outs, *args, micros=0.3):
    specs = [
        pl.BlockSpec(memory_space=pltpu.HBM if isinstance(a, tuple) else pltpu.VMEM) for a in args
    ]
    held = sum(math.prod(shape) * jnp.dtype(dtype).itemsize for shape, dtype in outs)
    return pl.pallas_call(
        kernel,
        in_specs=specs,
        out_specs=[pl.BlockSpec(memory_space=pltpu.VMEM)] * len(outs),
        out_shape=[pltpu.VMEM(shape, dtype) for shape, dtype in outs],
        scratch_shapes=[],
        cost_estimate=pl.CostEstimate(flops=int(micros * 1e8), transcendentals=0, bytes_accessed=held),
        compiler_params=pltpu.CompilerParams(vmem_limit_bytes=16 * 2**20),
    )(*(pltpu.with_memory_space_constraint(a[0], pltpu.HBM) if isinstance(a, tuple) else a for a in args))


def is_even():
    return lax.axis_index(AXIS) % 2 == 0


def on_right(level):
    return (lax.axis_index(AXIS) >> level) % 2 == 1


def split3(values):
    high = values.astype(BF16)
    rest = values - high.astype(F32)
    mid = rest.astype(BF16)
    low = (rest - mid.astype(F32)).astype(BF16)
    return high, mid, low


def dot(left, right):
    return jnp.dot(left, right, preferred_element_type=F32)


def fold(product, count):
    rows = product.shape[0] // count
    total = product[(count - 1) * rows :]
    for i in range(count - 2, -1, -1):
        total = total + product[i * rows : (i + 1) * rows]
    return total


def times_exact(parts, right):
    return fold(dot(jnp.concatenate(parts, 0), right), 3)


def times_split(parts, high, mid, low):
    small = dot(parts[0], low) + fold(dot(jnp.concatenate(parts[:2], 0), mid), 2)
    return fold(dot(jnp.concatenate(parts, 0), high), 3) + small


def gather_copies(pairs, sems):
    copies = [pltpu.make_async_copy(a, b, sems.at[i]) for i, (a, b) in enumerate(pairs)]
    for copy in copies:
        copy.start()
    return copies


def payload_kernel(x_hbm, u_hbm, l_hbm, near_ref, far_ref, chain_ref):
    even = is_even()
    width = chain_ref.shape[0]
    rows = x_hbm.shape[0]
    last = x_hbm.shape[1] - width

    def work(first, final, up, low, bottom, sems):
        head, tail = pl.ds(0, width), pl.ds(last, width)
        copies = gather_copies(
            [
                (x_hbm.at[:, head], first),
                (x_hbm.at[:, tail], final),
                (l_hbm.at[:, tail], bottom),
                (u_hbm.at[:, tail], up),
                (l_hbm.at[:, head], low),
            ],
            sems,
        )
        for copy in copies:
            copy.wait()
        for ref, here, there in ((near_ref, final, first), (far_ref, first, final)):
            for j, part in enumerate(split3(jnp.where(even, here[...], there[...]))):
                ref[pl.ds(j * rows, rows), :] = part
        chain = -bottom[...]
        chain_ref[...] = chain
        low_tip, up_tip = low[...].astype(F32), up[...].astype(F32)
        near_ref[pl.ds(3 * rows, width), :] = jnp.where(even, up_tip, low_tip).astype(BF16)
        far_ref[pl.ds(3 * rows, width), :] = jnp.where(even, low_tip, up_tip).astype(BF16)
        near_ref[pl.ds(3 * rows + width, width), :] = chain

    vec = pltpu.VMEM((rows, width), F32)
    mat = pltpu.VMEM(chain_ref.shape, BF16)
    pl.run_scoped(work, vec, vec, mat, mat, mat, pltpu.SemaphoreType.DMA((5,)))


def split_store(ref, rows, values):
    for j, part in enumerate(split3(values)):
        ref[j, rows, :] = part


def first_local_kernel(b_hbm, x_hbm, d_hbm, s_hbm, p_hbm, z_hbm, u_hbm, l_hbm, acc_ref, b_ref, x_ref, d3_ref, s3_ref, p3_ref, z_ref, u_ref, l_ref):
    width = d_hbm.shape[1]

    def work(d_ref, s_ref, p_ref, sems):
        copies = gather_copies(
            [(x_hbm, x_ref), (d_hbm, d_ref), (s_hbm, s_ref), (p_hbm, p_ref), (b_hbm, b_ref), (z_hbm, z_ref), (u_hbm, u_ref), (l_hbm, l_ref)],
            sems,
        )
        for copy in copies[:2]:
            copy.wait()
        for source, target, copy in ((d_ref, d3_ref, 2), (s_ref, s3_ref, 3), (p_ref, p3_ref, 4)):
            for k in range(d_ref.shape[0] // width):
                split_store(target, pl.ds(k * width, width), source[k * width : (k + 1) * width, :])
            copies[copy].wait()
        local_part(b_ref, x_ref, d3_ref, s3_ref, p3_ref, acc_ref)
        for copy in copies[5:]:
            copy.wait()

    mat = pltpu.VMEM(d_hbm.shape, F32)
    pl.run_scoped(work, mat, mat, mat, pltpu.SemaphoreType.DMA((8,)))


def local_part(b_ref, x_ref, d3_ref, s3_ref, p3_ref, acc_ref):
    width = d3_ref.shape[2]
    last = d3_ref.shape[1] // width - 1
    x = [split3(x_ref[:, k * width : (k + 1) * width]) for k in range(last + 1)]
    for k in range(last + 1):
        rows = pl.ds(k * width, width)
        part = times_split(x[k], *(d3_ref[j, rows, :] for j in range(3)))
        if k > 0:
            part = part + times_split(x[k - 1], *(s3_ref[j, rows, :] for j in range(3)))
        if k < last:
            part = part + times_split(x[k + 1], *(p3_ref[j, rows, :] for j in range(3)))
        acc_ref[:, k * width : (k + 1) * width] = b_ref[:, k * width : (k + 1) * width] - part


def choose(condition, left, right):
    return jnp.where(condition, left.astype(F32), right.astype(F32)).astype(left.dtype)


def sides_of(near_ref, far_ref, rows):
    even = is_even()
    if near_ref.dtype == F32:
        near, far = near_ref[...], far_ref[...]
        return split3(jnp.where(even, far, near)), split3(jnp.where(even, near, far))
    near = [near_ref[pl.ds(j * rows, rows), :] for j in range(3)]
    far = [far_ref[pl.ds(j * rows, rows), :] for j in range(3)]
    before = [choose(even, f, n) for n, f in zip(near, far)]
    after = [choose(even, n, f) for n, f in zip(near, far)]
    return before, after


def close_residual(acc_ref, near_ref, far_ref, s3_ref, p3_ref):
    width = s3_ref.shape[2]
    last = s3_ref.shape[1] - width
    before, after = sides_of(near_ref, far_ref, acc_ref.shape[0])
    first = acc_ref[:, :width] - times_split(before, *(s3_ref[j, :width, :] for j in range(3)))
    final = acc_ref[:, last:] - times_split(after, *(p3_ref[j, last:, :] for j in range(3)))
    return first, acc_ref[:, width:last], final


def squares(parts):
    total = None
    for part in parts:
        for i in range(0, part.shape[1], 128):
            piece = part[:, i : i + 128]
            total = piece * piece if total is None else total + piece * piece
    return total


def lane_row(total, turn, lanes):
    total = jnp.sum(total, axis=1, keepdims=True)
    rows = total.shape[0]
    row = lax.broadcasted_iota(jnp.int32, (rows, lanes), 0)
    lane = lax.broadcasted_iota(jnp.int32, (rows, lanes), 1)
    return jnp.sum(jnp.where(lane == row + turn * rows, total, 0.0), axis=0, keepdims=True)


def solve_kernel(acc_ref, near_ref, far_ref, s3_ref, p3_ref, z_ref, mix_ref, both_ref, top_ref, local_ref, norm_ref):
    parts = close_residual(acc_ref, near_ref, far_ref, s3_ref, p3_ref)
    width = s3_ref.shape[2]
    rows = acc_ref.shape[0]
    rounded = jnp.concatenate([p.astype(BF16) for p in parts], 1)
    local = dot(rounded, z_ref[...])
    local_ref[...] = local
    own_top = local[:, :width]
    mixed = times_split(split3(own_top), *(mix_ref[j] for j in range(3)))
    both_ref[:rows, :] = local[:, -width:] - mixed
    both_ref[rows:, :] = own_top
    top_ref[...] = own_top
    norm_ref[...] = squares(parts)


def norm_kernel(acc_ref, near_ref, far_ref, s3_ref, p3_ref, middle_ref, rest_ref, norm_ref, *, turn):
    first, _, final = close_residual(acc_ref, near_ref, far_ref, s3_ref, p3_ref)
    row = rest_ref[...] + lane_row(middle_ref[...] + squares((first, final)), turn, norm_ref.shape[1])
    norm_ref[...] = jnp.broadcast_to(row, norm_ref.shape)


def mix_kernel(near_ref, far_ref, chain_ref, before_ref, after_ref, mix_ref):
    even = is_even()
    width = chain_ref.shape[0]
    spikes = pl.ds(far_ref.shape[0] - width, width)
    near, far = near_ref[spikes, :], far_ref[spikes, :]
    before = choose(even, far, near)
    before_ref[...] = before
    after_ref[...] = choose(even, near, far)
    for j, part in enumerate(split3(dot(before, chain_ref[...]))):
        mix_ref[j] = part


def pair_kernel(own_ref, near_ref, second_ref, prefix_ref, whole_ref):
    right = on_right(0)
    width = own_ref.shape[0]
    own = own_ref[...].astype(F32)
    other = near_ref[pl.ds(near_ref.shape[0] - width, width), :].astype(F32)
    second = jnp.where(right, own, other).astype(BF16)
    first = jnp.where(right, other, own).astype(BF16)
    second_ref[...] = second
    row = lax.broadcasted_iota(jnp.int32, (width, width), 0)
    col = lax.broadcasted_iota(jnp.int32, (width, width), 1)
    prefix = jnp.where(right, other, jnp.where(row == col, 1.0, 0.0))
    for j, part in enumerate(split3(prefix)):
        prefix_ref[j] = part
    whole_ref[...] = dot(first, second)


def next_level(level, whole, other, prefix, second_ref, prefix_out, whole_out=None, half_out=None):
    right = on_right(level)
    second3 = split3(jnp.where(right, whole, other))
    first3 = split3(jnp.where(right, other, whole))
    for j, part in enumerate(second3):
        second_ref[j] = part
    product = None
    if whole_out is not None:
        product = times_split(first3, *second3)
        whole_out[...] = product
        if half_out is not None:
            half = half_out.shape[0]
            half_out[...] = jnp.where(is_even(), product[:half], product[half:])
    for j, part in enumerate(split3(times_split(first3, *prefix))):
        prefix_out[j] = choose(right, part, prefix[j])
    return product


def static_kernel(whole_ref, got_ref, twin_ref, prefix_ref, *outs, level):
    even = is_even()
    got, twin = got_ref[...], twin_ref[...]
    other = jnp.concatenate([jnp.where(even, got, twin), jnp.where(even, twin, got)], 0)
    next_level(level, whole_ref[...], other, parts_of(prefix_ref), *outs)


def chip_kernel(whole_ref, got_ref, twin_ref, prefix_ref, *outs):
    even = is_even()
    got, twin = got_ref[...], twin_ref[...]
    other = dot(choose(even, got, twin), choose(even, twin, got))
    next_level(1, whole_ref[...], other, parts_of(prefix_ref), *outs)


def merged(right, total, got, matrix):
    first = split3(jnp.where(right, got, total))
    product = times_split(first, *matrix) if isinstance(matrix, list) else times_exact(first, matrix)
    return product + jnp.where(right, total, got)


def parts_of(ref):
    return [ref[j] for j in range(3)]


def carry_step(level, values, reach_ref):
    return jnp.where(on_right(level), times_split(split3(values), *parts_of(reach_ref)), 0.0)


def sent_on(level, total, second_ref, carried_ref):
    product = times_split(split3(total), *parts_of(second_ref))
    carried_ref[...] = jnp.where(on_right(level), total, product)


def level0_kernel(both_ref, got_ref, second_ref, total_ref, carry_ref):
    right = on_right(0)
    rows = total_ref.shape[0]
    total, got = both_ref[:rows, :], got_ref[:rows, :]
    carry_ref[...] = jnp.where(right, got, 0.0)
    total_ref[...] = merged(right, total, got, second_ref[...])


def level0_wide_kernel(both_ref, got_ref, second_ref, next_ref, total_ref, carry_ref, carried_ref):
    level0_kernel(both_ref, got_ref, second_ref, total_ref, carry_ref)
    sent_on(1, total_ref[...], next_ref, carried_ref)


def level_kernel(total_ref, got_ref, carry_ref, reach_ref, second_ref, total_out, carry_out, *, level):
    got = got_ref[...]
    total_out[...] = merged(on_right(level), total_ref[...], got, parts_of(second_ref))
    carry_out[...] = carry_ref[...] + carry_step(level, got, reach_ref)


def wide_kernel(
    total_ref, carried_ref, got_ref, low_ref, cross_ref, carry_ref, reach_ref, reach2_ref, second_ref, second2_ref,
    *rest, level
):
    next_ref = rest[0] if len(rest) == 4 else None
    total_out, carry_out = rest[-3:-1] if next_ref is not None else rest
    right, right2 = on_right(level), on_right(level + 1)
    got, low = got_ref[...], low_ref[...] + cross_ref[...]
    carry_out[...] = carry_ref[...] + carry_step(level, got, reach_ref) + carry_step(level + 1, low, reach2_ref)
    passed = times_split(split3(got), *parts_of(second_ref))
    pair = jnp.where(right, passed + total_ref[...], carried_ref[...] + got)
    total = merged(right2, pair, low, parts_of(second2_ref))
    total_out[...] = total
    if next_ref is not None:
        sent_on(level + 2, total, next_ref, rest[-1])


def tips_kernel(*refs, level, wide):
    gots, refs = refs[: 3 if wide else 1], refs[3 if wide else 1 :]
    reaches, refs = refs[: 2 if wide else 1], refs[2 if wide else 1 :]
    carry_ref, near_ref, far_ref, local_ref, x_ref, u_ref, l_ref, before_ref, after_ref, chain_ref = refs[:10]
    top_out, previous_out, near_out, far_out = refs[10:]
    even = is_even()
    rows, width = carry_ref.shape
    carry = carry_ref[...] + carry_step(level, gots[0][...], reaches[0])
    if wide:
        carry = carry + carry_step(level + 1, gots[1][...] + gots[2][...], reaches[1])
    own_top = local_ref[:, :width]
    own_bottom = local_ref[:, -width:]
    next_top = jnp.where(even, near_ref[rows:, :], far_ref[...])
    offset = own_bottom - times_exact(split3(next_top), u_ref[:, -width:])
    previous = carry - times_exact(split3(own_top), before_ref[...])
    bottom = offset + times_exact(split3(previous), chain_ref[...])
    top = (next_top - times_exact(split3(bottom), after_ref[...])).astype(BF16)
    previous = previous.astype(BF16)
    top_out[...] = top
    previous_out[...] = previous

    def updated(columns):
        change = local_ref[:, columns] - dot(top, u_ref[:, columns]) - dot(previous, l_ref[:, columns])
        return x_ref[:, columns] + change

    size = x_ref.shape[1]
    first = updated(slice(0, width))
    final = updated(slice(size - width, size))
    near_out[...] = jnp.where(even, final, first)
    far_out[...] = jnp.where(even, first, final)


def update_kernel(top_ref, previous_ref, local_ref, x_ref, u_ref, l_ref, b_ref, d3_ref, s3_ref, p3_ref, *refs):
    x_out, acc_ref = refs[-2:] if len(refs) == 2 else refs[-4:-2]
    change = local_ref[...] - dot(top_ref[...], u_ref[...]) - dot(previous_ref[...], l_ref[...])
    x_out[...] = x_ref[...] + change
    local_part(b_ref, x_out, d3_ref, s3_ref, p3_ref, acc_ref)
    if len(refs) > 2:
        norms, middle_ref, row_ref = refs[:-4], refs[-2], refs[-1]
        width = d3_ref.shape[2]
        middle_ref[...] = squares((acc_ref[:, width : acc_ref.shape[1] - width],))
        row_ref[...] = sum(lane_row(ref[...], turn, row_ref.shape[1]) for turn, ref in enumerate(norms))


def finish_kernel(gathered_ref, out_ref, *, total):
    sums = jnp.sqrt(jnp.sum(gathered_ref[...], axis=0, keepdims=True) / total)
    rows = out_ref.shape[1]
    for turn in range(out_ref.shape[0]):
        out_ref[pl.ds(turn, 1), :] = sums[:, turn * rows : (turn + 1) * rows]


def body(
    right_sides,
    initial,
    diag_blocks,
    sub_blocks,
    super_blocks,
    local_inverse,
    upper_spikes,
    lower_spikes,
):
    width = diag_blocks.shape[1]
    rows, size = right_sides.shape
    count = lax.axis_size(AXIS)
    levels = (count - 1).bit_length()
    tip = ((rows, width), F32)
    low_tip = ((rows, width), BF16)
    square = ((width, width), F32)
    low_square = ((width, width), BF16)
    triple = ((3, width, width), BF16)
    half = ((width // 2, width), F32)
    wide = ((rows, size), F32)
    big = ((3, size, width), BF16)
    lanes = -(-rows * (ITERS + 1) // 128) * 128

    near_pack, far_pack, chain = kernel_call(
        payload_kernel,
        [((3 * rows + 2 * width, width), BF16), ((3 * rows + width, width), BF16), low_square],
        (initial,), (upper_spikes,), (lower_spikes,),
    )
    near = exchange(near_pack, 1)
    far = across(far_pack)
    acc, right_sides, solution, d3, s3, p3, local_inverse, upper_spikes, lower_spikes = kernel_call(
        first_local_kernel,
        [wide, wide, wide, big, big, big, (local_inverse.shape, BF16), (upper_spikes.shape, BF16), (lower_spikes.shape, BF16)],
        *((a,) for a in (right_sides, initial, diag_blocks, sub_blocks, super_blocks, local_inverse, upper_spikes, lower_spikes)),
        micros=3,
    )
    before, after, mix = kernel_call(mix_kernel, [low_square, low_square, triple], near, far, chain)

    second, prefix, whole = kernel_call(pair_kernel, [low_square, triple, square], chain, near)
    seconds, reaches = [second], [None, prefix]
    for level in range(1, levels - 1):
        got = exchange(chain if level == 1 else piece, 1 << level)
        twin = exchange(got, 1)
        kernel = chip_kernel if level == 1 else functools.partial(static_kernel, level=level)
        second, prefix, *rest = kernel_call(
            kernel, [triple, triple] + [square, half] * (level < levels - 2), whole, got, twin, prefix, micros=1
        )
        if rest:
            whole, piece = rest
        seconds.append(second)
        reaches.append(prefix)

    norms = []
    for turn in range(ITERS):
        both, own_top, local, norm = kernel_call(
            solve_kernel, [((2 * rows, width), F32), tip, wide, ((rows, 128), F32)],
            acc, near, far, s3, p3, local_inverse, mix, micros=0.8,
        )
        norms.append(norm)
        swapped = exchange(both, 1)
        far_top = across(own_top)
        groups = [(0, 1)]
        while sum(groups[-1]) < levels:
            level = sum(groups[-1])
            groups.append((level, 2 if turn > 0 and level + 2 <= levels else 1))
        carried = None
        for i, (level, size_of) in enumerate(groups[:-1]):
            after_size = groups[i + 1][1]
            outs = [tip, tip] + [tip] * (after_size == 2)
            following = [seconds[level + size_of]] if after_size == 2 else []
            if level == 0:
                kernel = level0_wide_kernel if after_size == 2 else level0_kernel
                total, carry, *more = kernel_call(kernel, outs, both, swapped, seconds[0], *following)
            elif size_of == 1:
                got = exchange(total, 1 << level)
                total, carry, *more = kernel_call(
                    functools.partial(level_kernel, level=level), outs, total, got, carry, reaches[level], seconds[level]
                )
            else:
                step = 1 << level
                got = exchange(total, step)
                low = exchange(carried, 2 * step)
                cross = exchange(carried, 3 * step)
                total, carry, *more = kernel_call(
                    functools.partial(wide_kernel, level=level), outs, total, carried, got, low, cross, carry,
                    reaches[level], reaches[level + 1], seconds[level], seconds[level + 1], *following,
                )
            carried = more[0] if more else None
        level, size_of = groups[-1]
        gots = [exchange(total, 1 << level)]
        if size_of == 2:
            gots.append(exchange(carried, 2 << level))
            gots.append(exchange(carried, 3 << level))
        top, previous, near, far = kernel_call(
            functools.partial(tips_kernel, level=level, wide=size_of == 2), [low_tip, low_tip, tip, tip],
            *gots, *reaches[level : level + size_of], carry, swapped, far_top, local, solution, upper_spikes, lower_spikes,
            before, after, chain, micros=1,
        )
        near = exchange(near, 1)
        far = across(far)
        final = turn == ITERS - 1
        solution, acc, *sums = kernel_call(
            update_kernel, [wide, wide] + [((rows, 128), F32), ((1, lanes), F32)] * final,
            top, previous, local, solution, upper_spikes, lower_spikes, right_sides, d3, s3, p3, *(norms if final else ()),
            micros=1,
        )
    mine = kernel_call(
        functools.partial(norm_kernel, turn=ITERS), [((count, lanes), F32)], acc, near, far, s3, p3, *sums
    )[0]
    gathered = lax.all_to_all(mine, AXIS, 0, 0, tiled=True)
    result = pl.pallas_call(
        functools.partial(finish_kernel, total=size * count), out_shape=jax.ShapeDtypeStruct((ITERS + 1, rows), F32),
        compiler_params=pltpu.CompilerParams(vmem_limit_bytes=16 * 2**20),
    )(gathered)
    return solution, result


def solution(mesh):
    return jax.shard_map(
        body,
        mesh=mesh,
        in_specs=(
            P(None, AXIS),
            P(None, AXIS),
            P(AXIS, None),
            P(AXIS, None),
            P(AXIS, None),
            P(AXIS, None),
            P(None, AXIS),
            P(None, AXIS),
        ),
        out_specs=(P(None, AXIS), P()),
        check_vma=False,
    )
```

```python
import functools
import math

import jax
import jax.numpy as jnp
from jax import lax
from jax.experimental import pallas as pl
from jax.experimental.pallas import tpu as pltpu
from jax.sharding import PartitionSpec as P


ITERS = 2
AXIS = "rows"
F32 = jnp.float32
BF16 = jnp.bfloat16


def exchange(values, distance):
    count = lax.axis_size(AXIS)
    return lax.ppermute(values, AXIS, [(i, i ^ distance) for i in range(count)])


def across(values):
    count = lax.axis_size(AXIS)
    pairs = [(i, i + 1) for i in range(1, count - 1, 2)]
    return lax.ppermute(values, AXIS, pairs + [(b, a) for a, b in pairs])


def kernel_call(kernel, outs, *args, micros=0.3):
    specs = [
        pl.BlockSpec(memory_space=pltpu.HBM if isinstance(a, tuple) else pltpu.VMEM) for a in args
    ]
    held = sum(math.prod(shape) * jnp.dtype(dtype).itemsize for shape, dtype in outs)
    return pl.pallas_call(
        kernel,
        in_specs=specs,
        out_specs=[pl.BlockSpec(memory_space=pltpu.VMEM)] * len(outs),
        out_shape=[pltpu.VMEM(shape, dtype) for shape, dtype in outs],
        scratch_shapes=[],
        cost_estimate=pl.CostEstimate(flops=int(micros * 1e8), transcendentals=0, bytes_accessed=held),
        compiler_params=pltpu.CompilerParams(vmem_limit_bytes=16 * 2**20),
    )(*(pltpu.with_memory_space_constraint(a[0], pltpu.HBM) if isinstance(a, tuple) else a for a in args))


def is_even():
    return lax.axis_index(AXIS) % 2 == 0


def on_right(level):
    return (lax.axis_index(AXIS) >> level) % 2 == 1


def split3(values):
    high = values.astype(BF16)
    rest = values - high.astype(F32)
    mid = rest.astype(BF16)
    low = (rest - mid.astype(F32)).astype(BF16)
    return high, mid, low


def dot(left, right):
    return jnp.dot(left, right, preferred_element_type=F32)


def fold(product, count):
    rows = product.shape[0] // count
    total = product[(count - 1) * rows :]
    for i in range(count - 2, -1, -1):
        total = total + product[i * rows : (i + 1) * rows]
    return total


def times_exact(parts, right):
    return fold(dot(jnp.concatenate(parts, 0), right), 3)


def times_split(parts, high, mid, low):
    small = dot(parts[0], low) + fold(dot(jnp.concatenate(parts[:2], 0), mid), 2)
    return fold(dot(jnp.concatenate(parts, 0), high), 3) + small


def gather_copies(pairs, sems):
    copies = [pltpu.make_async_copy(a, b, sems.at[i]) for i, (a, b) in enumerate(pairs)]
    for copy in copies:
        copy.start()
    return copies


def payload_kernel(x_hbm, u_hbm, l_hbm, near_ref, far_ref, chain_ref):
    even = is_even()
    width = chain_ref.shape[0]
    rows = x_hbm.shape[0]
    last = x_hbm.shape[1] - width

    def work(first, final, up, low, bottom, sems):
        head, tail = pl.ds(0, width), pl.ds(last, width)
        copies = gather_copies(
            [
                (x_hbm.at[:, head], first),
                (x_hbm.at[:, tail], final),
                (l_hbm.at[:, tail], bottom),
                (u_hbm.at[:, tail], up),
                (l_hbm.at[:, head], low),
            ],
            sems,
        )
        for copy in copies:
            copy.wait()
        for ref, here, there in ((near_ref, final, first), (far_ref, first, final)):
            for j, part in enumerate(split3(jnp.where(even, here[...], there[...]))):
                ref[pl.ds(j * rows, rows), :] = part
        chain = -bottom[...]
        chain_ref[...] = chain
        low_tip, up_tip = low[...].astype(F32), up[...].astype(F32)
        near_ref[pl.ds(3 * rows, width), :] = jnp.where(even, up_tip, low_tip).astype(BF16)
        far_ref[pl.ds(3 * rows, width), :] = jnp.where(even, low_tip, up_tip).astype(BF16)
        near_ref[pl.ds(3 * rows + width, width), :] = chain

    vec = pltpu.VMEM((rows, width), F32)
    mat = pltpu.VMEM(chain_ref.shape, BF16)
    pl.run_scoped(work, vec, vec, mat, mat, mat, pltpu.SemaphoreType.DMA((5,)))


def split_store(ref, rows, values):
    for j, part in enumerate(split3(values)):
        ref[j, rows, :] = part


def first_local_kernel(b_hbm, x_hbm, d_hbm, s_hbm, p_hbm, acc_ref, b_ref, x_ref, d3_ref, s3_ref, p3_ref):
    width = d_hbm.shape[1]

    def work(d_ref, s_ref, p_ref, sems):
        copies = gather_copies(
            [(x_hbm, x_ref), (d_hbm, d_ref), (s_hbm, s_ref), (p_hbm, p_ref), (b_hbm, b_ref)],
            sems,
        )
        for copy in copies[:2]:
            copy.wait()
        for source, target, copy in ((d_ref, d3_ref, 2), (s_ref, s3_ref, 3), (p_ref, p3_ref, 4)):
            for k in range(d_ref.shape[0] // width):
                split_store(target, pl.ds(k * width, width), source[k * width : (k + 1) * width, :])
            copies[copy].wait()
        local_part(b_ref, x_ref, d3_ref, s3_ref, p3_ref, acc_ref)

    mat = pltpu.VMEM(d_hbm.shape, F32)
    pl.run_scoped(work, mat, mat, mat, pltpu.SemaphoreType.DMA((5,)))


def local_part(b_ref, x_ref, d3_ref, s3_ref, p3_ref, acc_ref):
    width = d3_ref.shape[2]
    last = d3_ref.shape[1] // width - 1
    x = [split3(x_ref[:, k * width : (k + 1) * width]) for k in range(last + 1)]
    for k in range(last + 1):
        rows = pl.ds(k * width, width)
        part = times_split(x[k], *(d3_ref[j, rows, :] for j in range(3)))
        if k > 0:
            part = part + times_split(x[k - 1], *(s3_ref[j, rows, :] for j in range(3)))
        if k < last:
            part = part + times_split(x[k + 1], *(p3_ref[j, rows, :] for j in range(3)))
        acc_ref[:, k * width : (k + 1) * width] = b_ref[:, k * width : (k + 1) * width] - part


def choose(condition, left, right):
    return jnp.where(condition, left.astype(F32), right.astype(F32)).astype(left.dtype)


def sides_of(near_ref, far_ref, rows):
    even = is_even()
    if near_ref.dtype == F32:
        near, far = near_ref[...], far_ref[...]
        return split3(jnp.where(even, far, near)), split3(jnp.where(even, near, far))
    near = [near_ref[pl.ds(j * rows, rows), :] for j in range(3)]
    far = [far_ref[pl.ds(j * rows, rows), :] for j in range(3)]
    before = [choose(even, f, n) for n, f in zip(near, far)]
    after = [choose(even, n, f) for n, f in zip(near, far)]
    return before, after


def close_residual(acc_ref, near_ref, far_ref, s3_ref, p3_ref):
    width = s3_ref.shape[2]
    last = s3_ref.shape[1] - width
    before, after = sides_of(near_ref, far_ref, acc_ref.shape[0])
    first = acc_ref[:, :width] - times_split(before, *(s3_ref[j, :width, :] for j in range(3)))
    final = acc_ref[:, last:] - times_split(after, *(p3_ref[j, last:, :] for j in range(3)))
    return first, acc_ref[:, width:last], final


def squares(parts):
    total = None
    for part in parts:
        for i in range(0, part.shape[1], 128):
            piece = part[:, i : i + 128]
            total = piece * piece if total is None else total + piece * piece
    return total


def lane_row(total, turn, lanes):
    total = jnp.sum(total, axis=1, keepdims=True)
    rows = total.shape[0]
    row = lax.broadcasted_iota(jnp.int32, (rows, lanes), 0)
    lane = lax.broadcasted_iota(jnp.int32, (rows, lanes), 1)
    return jnp.sum(jnp.where(lane == row + turn * rows, total, 0.0), axis=0, keepdims=True)


def solve_kernel(acc_ref, near_ref, far_ref, s3_ref, p3_ref, z_ref, mix_ref, both_ref, top_ref, local_ref, norm_ref):
    parts = close_residual(acc_ref, near_ref, far_ref, s3_ref, p3_ref)
    width = s3_ref.shape[2]
    rows = acc_ref.shape[0]
    rounded = jnp.concatenate([p.astype(BF16) for p in parts], 1)
    local = dot(rounded, z_ref[...])
    local_ref[...] = local
    own_top = local[:, :width]
    mixed = times_split(split3(own_top), *(mix_ref[j] for j in range(3)))
    both_ref[:rows, :] = local[:, -width:] - mixed
    both_ref[rows:, :] = own_top
    top_ref[...] = own_top
    norm_ref[...] = squares(parts)


def norm_kernel(acc_ref, near_ref, far_ref, s3_ref, p3_ref, middle_ref, rest_ref, norm_ref, *, turn):
    first, _, final = close_residual(acc_ref, near_ref, far_ref, s3_ref, p3_ref)
    row = rest_ref[...] + lane_row(middle_ref[...] + squares((first, final)), turn, norm_ref.shape[1])
    norm_ref[...] = jnp.broadcast_to(row, norm_ref.shape)


def mix_kernel(near_ref, far_ref, chain_ref, before_ref, after_ref, mix_ref):
    even = is_even()
    width = chain_ref.shape[0]
    spikes = pl.ds(far_ref.shape[0] - width, width)
    near, far = near_ref[spikes, :], far_ref[spikes, :]
    before = choose(even, far, near)
    before_ref[...] = before
    after_ref[...] = choose(even, near, far)
    for j, part in enumerate(split3(dot(before, chain_ref[...]))):
        mix_ref[j] = part


def pair_kernel(own_ref, near_ref, second_ref, prefix_ref, whole_ref):
    right = on_right(0)
    width = own_ref.shape[0]
    own = own_ref[...].astype(F32)
    other = near_ref[pl.ds(near_ref.shape[0] - width, width), :].astype(F32)
    second = jnp.where(right, own, other).astype(BF16)
    first = jnp.where(right, other, own).astype(BF16)
    second_ref[...] = second
    row = lax.broadcasted_iota(jnp.int32, (width, width), 0)
    col = lax.broadcasted_iota(jnp.int32, (width, width), 1)
    prefix = jnp.where(right, other, jnp.where(row == col, 1.0, 0.0))
    for j, part in enumerate(split3(prefix)):
        prefix_ref[j] = part
    whole_ref[...] = dot(first, second)


def next_level(level, whole, other, prefix, second_ref, prefix_out, whole_out=None, half_out=None):
    right = on_right(level)
    second3 = split3(jnp.where(right, whole, other))
    first3 = split3(jnp.where(right, other, whole))
    for j, part in enumerate(second3):
        second_ref[j] = part
    product = None
    if whole_out is not None:
        product = times_split(first3, *second3)
        whole_out[...] = product
        if half_out is not None:
            half = half_out.shape[0]
            half_out[...] = jnp.where(is_even(), product[:half], product[half:])
    for j, part in enumerate(split3(times_split(first3, *prefix))):
        prefix_out[j] = choose(right, part, prefix[j])
    return product


def static_kernel(whole_ref, got_ref, twin_ref, prefix_ref, *outs, level):
    even = is_even()
    got, twin = got_ref[...], twin_ref[...]
    other = jnp.concatenate([jnp.where(even, got, twin), jnp.where(even, twin, got)], 0)
    next_level(level, whole_ref[...], other, parts_of(prefix_ref), *outs)


def chip_kernel(whole_ref, got_ref, twin_ref, prefix_ref, *outs):
    even = is_even()
    got, twin = got_ref[...], twin_ref[...]
    other = dot(choose(even, got, twin), choose(even, twin, got))
    next_level(1, whole_ref[...], other, parts_of(prefix_ref), *outs)


def merged(right, total, got, matrix):
    first = split3(jnp.where(right, got, total))
    product = times_split(first, *matrix) if isinstance(matrix, list) else times_exact(first, matrix)
    return product + jnp.where(right, total, got)


def parts_of(ref):
    return [ref[j] for j in range(3)]


def carry_step(level, values, reach_ref):
    return jnp.where(on_right(level), times_split(split3(values), *parts_of(reach_ref)), 0.0)


def sent_on(level, total, second_ref, carried_ref):
    product = times_split(split3(total), *parts_of(second_ref))
    carried_ref[...] = jnp.where(on_right(level), total, product)


def level0_kernel(both_ref, got_ref, second_ref, total_ref, carry_ref):
    right = on_right(0)
    rows = total_ref.shape[0]
    total, got = both_ref[:rows, :], got_ref[:rows, :]
    carry_ref[...] = jnp.where(right, got, 0.0)
    total_ref[...] = merged(right, total, got, second_ref[...])


def level0_wide_kernel(both_ref, got_ref, second_ref, next_ref, total_ref, carry_ref, carried_ref):
    level0_kernel(both_ref, got_ref, second_ref, total_ref, carry_ref)
    sent_on(1, total_ref[...], next_ref, carried_ref)


def level_kernel(total_ref, got_ref, carry_ref, reach_ref, second_ref, total_out, carry_out, *, level):
    got = got_ref[...]
    total_out[...] = merged(on_right(level), total_ref[...], got, parts_of(second_ref))
    carry_out[...] = carry_ref[...] + carry_step(level, got, reach_ref)


def wide_kernel(
    total_ref, carried_ref, got_ref, low_ref, cross_ref, carry_ref, reach_ref, reach2_ref, second_ref, second2_ref,
    *rest, level
):
    next_ref = rest[0] if len(rest) == 4 else None
    total_out, carry_out = rest[-3:-1] if next_ref is not None else rest
    right, right2 = on_right(level), on_right(level + 1)
    got, low = got_ref[...], low_ref[...] + cross_ref[...]
    carry_out[...] = carry_ref[...] + carry_step(level, got, reach_ref) + carry_step(level + 1, low, reach2_ref)
    passed = times_split(split3(got), *parts_of(second_ref))
    pair = jnp.where(right, passed + total_ref[...], carried_ref[...] + got)
    total = merged(right2, pair, low, parts_of(second2_ref))
    total_out[...] = total
    if next_ref is not None:
        sent_on(level + 2, total, next_ref, rest[-1])


def tips_kernel(*refs, level, wide):
    gots, refs = refs[: 3 if wide else 1], refs[3 if wide else 1 :]
    reaches, refs = refs[: 2 if wide else 1], refs[2 if wide else 1 :]
    carry_ref, near_ref, far_ref, local_ref, x_ref, u_ref, l_ref, before_ref, after_ref, chain_ref = refs[:10]
    top_out, previous_out, near_out, far_out = refs[10:]
    even = is_even()
    rows, width = carry_ref.shape
    carry = carry_ref[...] + carry_step(level, gots[0][...], reaches[0])
    if wide:
        carry = carry + carry_step(level + 1, gots[1][...] + gots[2][...], reaches[1])
    own_top = local_ref[:, :width]
    own_bottom = local_ref[:, -width:]
    next_top = jnp.where(even, near_ref[rows:, :], far_ref[...])
    offset = own_bottom - times_exact(split3(next_top), u_ref[:, -width:])
    previous = carry - times_exact(split3(own_top), before_ref[...])
    bottom = offset + times_exact(split3(previous), chain_ref[...])
    top = (next_top - times_exact(split3(bottom), after_ref[...])).astype(BF16)
    previous = previous.astype(BF16)
    top_out[...] = top
    previous_out[...] = previous

    def updated(columns):
        change = local_ref[:, columns] - dot(top, u_ref[:, columns]) - dot(previous, l_ref[:, columns])
        return x_ref[:, columns] + change

    size = x_ref.shape[1]
    first = updated(slice(0, width))
    final = updated(slice(size - width, size))
    near_out[...] = jnp.where(even, final, first)
    far_out[...] = jnp.where(even, first, final)


def update_kernel(top_ref, previous_ref, local_ref, x_ref, u_ref, l_ref, b_ref, d3_ref, s3_ref, p3_ref, *refs):
    x_out, acc_ref = refs[-2:] if len(refs) == 2 else refs[-4:-2]
    change = local_ref[...] - dot(top_ref[...], u_ref[...]) - dot(previous_ref[...], l_ref[...])
    x_out[...] = x_ref[...] + change
    local_part(b_ref, x_out, d3_ref, s3_ref, p3_ref, acc_ref)
    if len(refs) > 2:
        norms, middle_ref, row_ref = refs[:-4], refs[-2], refs[-1]
        width = d3_ref.shape[2]
        middle_ref[...] = squares((acc_ref[:, width : acc_ref.shape[1] - width],))
        row_ref[...] = sum(lane_row(ref[...], turn, row_ref.shape[1]) for turn, ref in enumerate(norms))


def finish_kernel(gathered_ref, out_ref, *, total):
    sums = jnp.sqrt(jnp.sum(gathered_ref[...], axis=0, keepdims=True) / total)
    rows = out_ref.shape[1]
    for turn in range(out_ref.shape[0]):
        out_ref[pl.ds(turn, 1), :] = sums[:, turn * rows : (turn + 1) * rows]


def body(
    right_sides,
    initial,
    diag_blocks,
    sub_blocks,
    super_blocks,
    local_inverse,
    upper_spikes,
    lower_spikes,
):
    width = diag_blocks.shape[1]
    rows, size = right_sides.shape
    count = lax.axis_size(AXIS)
    levels = (count - 1).bit_length()
    tip = ((rows, width), F32)
    low_tip = ((rows, width), BF16)
    square = ((width, width), F32)
    low_square = ((width, width), BF16)
    triple = ((3, width, width), BF16)
    half = ((width // 2, width), F32)
    wide = ((rows, size), F32)
    big = ((3, size, width), BF16)
    lanes = -(-rows * (ITERS + 1) // 128) * 128

    near_pack, far_pack, chain = kernel_call(
        payload_kernel,
        [((3 * rows + 2 * width, width), BF16), ((3 * rows + width, width), BF16), low_square],
        (initial,), (upper_spikes,), (lower_spikes,),
    )
    near = exchange(near_pack, 1)
    far = across(far_pack)
    acc, right_sides, solution, d3, s3, p3 = kernel_call(
        first_local_kernel, [wide, wide, wide, big, big, big],
        *((a,) for a in (right_sides, initial, diag_blocks, sub_blocks, super_blocks)), micros=3,
    )
    before, after, mix = kernel_call(mix_kernel, [low_square, low_square, triple], near, far, chain)

    second, prefix, whole = kernel_call(pair_kernel, [low_square, triple, square], chain, near)
    seconds, reaches = [second], [None, prefix]
    for level in range(1, levels - 1):
        got = exchange(chain if level == 1 else piece, 1 << level)
        twin = exchange(got, 1)
        kernel = chip_kernel if level == 1 else functools.partial(static_kernel, level=level)
        second, prefix, *rest = kernel_call(
            kernel, [triple, triple] + [square, half] * (level < levels - 2), whole, got, twin, prefix, micros=1
        )
        if rest:
            whole, piece = rest
        seconds.append(second)
        reaches.append(prefix)

    norms = []
    for turn in range(ITERS):
        both, own_top, local, norm = kernel_call(
            solve_kernel, [((2 * rows, width), F32), tip, wide, ((rows, 128), F32)],
            acc, near, far, s3, p3, local_inverse, mix, micros=0.8,
        )
        norms.append(norm)
        swapped = exchange(both, 1)
        far_top = across(own_top)
        groups = [(0, 1)]
        while sum(groups[-1]) < levels:
            level = sum(groups[-1])
            groups.append((level, 2 if turn > 0 and level + 2 <= levels else 1))
        carried = None
        for i, (level, size_of) in enumerate(groups[:-1]):
            after_size = groups[i + 1][1]
            outs = [tip, tip] + [tip] * (after_size == 2)
            following = [seconds[level + size_of]] if after_size == 2 else []
            if level == 0:
                kernel = level0_wide_kernel if after_size == 2 else level0_kernel
                total, carry, *more = kernel_call(kernel, outs, both, swapped, seconds[0], *following)
            elif size_of == 1:
                got = exchange(total, 1 << level)
                total, carry, *more = kernel_call(
                    functools.partial(level_kernel, level=level), outs, total, got, carry, reaches[level], seconds[level]
                )
            else:
                step = 1 << level
                got = exchange(total, step)
                low = exchange(carried, 2 * step)
                cross = exchange(carried, 3 * step)
                total, carry, *more = kernel_call(
                    functools.partial(wide_kernel, level=level), outs, total, carried, got, low, cross, carry,
                    reaches[level], reaches[level + 1], seconds[level], seconds[level + 1], *following,
                )
            carried = more[0] if more else None
        level, size_of = groups[-1]
        gots = [exchange(total, 1 << level)]
        if size_of == 2:
            gots.append(exchange(carried, 2 << level))
            gots.append(exchange(carried, 3 << level))
        top, previous, near, far = kernel_call(
            functools.partial(tips_kernel, level=level, wide=size_of == 2), [low_tip, low_tip, tip, tip],
            *gots, *reaches[level : level + size_of], carry, swapped, far_top, local, solution, upper_spikes, lower_spikes,
            before, after, chain, micros=1,
        )
        near = exchange(near, 1)
        far = across(far)
        final = turn == ITERS - 1
        solution, acc, *sums = kernel_call(
            update_kernel, [wide, wide] + [((rows, 128), F32), ((1, lanes), F32)] * final,
            top, previous, local, solution, upper_spikes, lower_spikes, right_sides, d3, s3, p3, *(norms if final else ()),
            micros=1,
        )
    mine = kernel_call(
        functools.partial(norm_kernel, turn=ITERS), [((count, lanes), F32)], acc, near, far, s3, p3, *sums
    )[0]
    gathered = lax.all_to_all(mine, AXIS, 0, 0, tiled=True)
    result = pl.pallas_call(
        functools.partial(finish_kernel, total=size * count), out_shape=jax.ShapeDtypeStruct((ITERS + 1, rows), F32),
        compiler_params=pltpu.CompilerParams(vmem_limit_bytes=16 * 2**20),
    )(gathered)
    return solution, result


def solution(mesh):
    return jax.shard_map(
        body,
        mesh=mesh,
        in_specs=(
            P(None, AXIS),
            P(None, AXIS),
            P(AXIS, None),
            P(AXIS, None),
            P(AXIS, None),
            P(AXIS, None),
            P(None, AXIS),
            P(None, AXIS),
        ),
        out_specs=(P(None, AXIS), P()),
        check_vma=False,
    )
```

```python
import functools
import math

import jax
import jax.numpy as jnp
from jax import lax
from jax.experimental import pallas as pl
from jax.experimental.pallas import tpu as pltpu
from jax.sharding import PartitionSpec as P


ITERS = 2
AXIS = "rows"
F32 = jnp.float32
BF16 = jnp.bfloat16


def exchange(values, distance):
    count = lax.axis_size(AXIS)
    return lax.ppermute(values, AXIS, [(i, i ^ distance) for i in range(count)])


def across(values):
    count = lax.axis_size(AXIS)
    pairs = [(i, i + 1) for i in range(1, count - 1, 2)]
    return lax.ppermute(values, AXIS, pairs + [(b, a) for a, b in pairs])


def kernel_call(kernel, outs, *args, micros=0.3):
    specs = [
        pl.BlockSpec(memory_space=pltpu.HBM if isinstance(a, tuple) else pltpu.VMEM) for a in args
    ]
    held = sum(math.prod(shape) * jnp.dtype(dtype).itemsize for shape, dtype in outs)
    return pl.pallas_call(
        kernel,
        in_specs=specs,
        out_specs=[pl.BlockSpec(memory_space=pltpu.VMEM)] * len(outs),
        out_shape=[pltpu.VMEM(shape, dtype) for shape, dtype in outs],
        scratch_shapes=[],
        cost_estimate=pl.CostEstimate(flops=int(micros * 1e8), transcendentals=0, bytes_accessed=held),
        compiler_params=pltpu.CompilerParams(vmem_limit_bytes=16 * 2**20),
    )(*(pltpu.with_memory_space_constraint(a[0], pltpu.HBM) if isinstance(a, tuple) else a for a in args))


def is_even():
    return lax.axis_index(AXIS) % 2 == 0


def on_right(level):
    return (lax.axis_index(AXIS) >> level) % 2 == 1


def split3(values):
    high = values.astype(BF16)
    rest = values - high.astype(F32)
    mid = rest.astype(BF16)
    low = (rest - mid.astype(F32)).astype(BF16)
    return high, mid, low


def dot(left, right):
    return jnp.dot(left, right, preferred_element_type=F32)


def fold(product, count):
    rows = product.shape[0] // count
    total = product[(count - 1) * rows :]
    for i in range(count - 2, -1, -1):
        total = total + product[i * rows : (i + 1) * rows]
    return total


def times_exact(parts, right):
    return fold(dot(jnp.concatenate(parts, 0), right), 3)


def times_split(parts, high, mid, low):
    small = dot(parts[0], low) + fold(dot(jnp.concatenate(parts[:2], 0), mid), 2)
    return fold(dot(jnp.concatenate(parts, 0), high), 3) + small


def gather_copies(pairs, sems):
    copies = [pltpu.make_async_copy(a, b, sems.at[i]) for i, (a, b) in enumerate(pairs)]
    for copy in copies:
        copy.start()
    return copies


def payload_kernel(x_hbm, u_hbm, l_hbm, near_ref, far_ref, chain_ref):
    even = is_even()
    width = chain_ref.shape[0]
    rows = x_hbm.shape[0]
    last = x_hbm.shape[1] - width

    def work(first, final, up, low, bottom, sems):
        head, tail = pl.ds(0, width), pl.ds(last, width)
        copies = gather_copies(
            [
                (x_hbm.at[:, head], first),
                (x_hbm.at[:, tail], final),
                (l_hbm.at[:, tail], bottom),
                (u_hbm.at[:, tail], up),
                (l_hbm.at[:, head], low),
            ],
            sems,
        )
        for copy in copies:
            copy.wait()
        for ref, here, there in ((near_ref, final, first), (far_ref, first, final)):
            for j, part in enumerate(split3(jnp.where(even, here[...], there[...]))):
                ref[pl.ds(j * rows, rows), :] = part
        chain = -bottom[...]
        chain_ref[...] = chain
        low_tip, up_tip = low[...].astype(F32), up[...].astype(F32)
        near_ref[pl.ds(3 * rows, width), :] = jnp.where(even, up_tip, low_tip).astype(BF16)
        far_ref[pl.ds(3 * rows, width), :] = jnp.where(even, low_tip, up_tip).astype(BF16)
        near_ref[pl.ds(3 * rows + width, width), :] = chain

    vec = pltpu.VMEM((rows, width), F32)
    mat = pltpu.VMEM(chain_ref.shape, BF16)
    pl.run_scoped(work, vec, vec, mat, mat, mat, pltpu.SemaphoreType.DMA((5,)))


def split_store(ref, rows, values):
    for j, part in enumerate(split3(values)):
        ref[j, rows, :] = part


def first_local_kernel(
    b_hbm, x_hbm, d_hbm, s_hbm, p_hbm, z_hbm, u_hbm, l_hbm, acc_ref, b_ref, x_ref, d3_ref, s3_ref, p3_ref, z_ref, u_ref, l_ref
):
    width = d_hbm.shape[1]
    blocks = d_hbm.shape[0] // width

    def work(d_ref, s_ref, p_ref, sems):
        pairs = [(x_hbm, x_ref), (b_hbm, b_ref)]
        for k in range(blocks):
            rows = pl.ds(k * width, width)
            pairs += [(a.at[rows, :], v.at[rows, :]) for a, v in ((d_hbm, d_ref), (s_hbm, s_ref), (p_hbm, p_ref))]
        pairs += [(z_hbm, z_ref), (u_hbm, u_ref), (l_hbm, l_ref)]
        copies = gather_copies(pairs, sems)
        copies[0].wait()
        copies[1].wait()
        for k in range(blocks):
            for j, (source, target) in enumerate(((d_ref, d3_ref), (s_ref, s3_ref), (p_ref, p3_ref))):
                copies[2 + 3 * k + j].wait()
                split_store(target, pl.ds(k * width, width), source[k * width : (k + 1) * width, :])
            local_block(k, b_ref, x_ref, d3_ref, s3_ref, p3_ref, acc_ref)
        for copy in copies[-3:]:
            copy.wait()

    mat = pltpu.VMEM(d_hbm.shape, F32)
    pl.run_scoped(work, mat, mat, mat, pltpu.SemaphoreType.DMA((5 + 3 * blocks,)))


def local_block(k, b_ref, x_ref, d3_ref, s3_ref, p3_ref, acc_ref):
    width = d3_ref.shape[2]
    last = d3_ref.shape[1] // width - 1
    rows = pl.ds(k * width, width)

    def term(i, ref):
        return times_split(split3(x_ref[:, i * width : (i + 1) * width]), *(ref[j, rows, :] for j in range(3)))

    part = term(k, d3_ref)
    if k > 0:
        part = part + term(k - 1, s3_ref)
    if k < last:
        part = part + term(k + 1, p3_ref)
    acc_ref[:, k * width : (k + 1) * width] = b_ref[:, k * width : (k + 1) * width] - part


def local_part(b_ref, x_ref, d3_ref, s3_ref, p3_ref, acc_ref):
    for k in range(d3_ref.shape[1] // d3_ref.shape[2]):
        local_block(k, b_ref, x_ref, d3_ref, s3_ref, p3_ref, acc_ref)


def choose(condition, left, right):
    return jnp.where(condition, left.astype(F32), right.astype(F32)).astype(left.dtype)


def sides_of(near_ref, far_ref, rows):
    even = is_even()
    if near_ref.dtype == F32:
        near, far = near_ref[...], far_ref[...]
        return split3(jnp.where(even, far, near)), split3(jnp.where(even, near, far))
    near = [near_ref[pl.ds(j * rows, rows), :] for j in range(3)]
    far = [far_ref[pl.ds(j * rows, rows), :] for j in range(3)]
    before = [choose(even, f, n) for n, f in zip(near, far)]
    after = [choose(even, n, f) for n, f in zip(near, far)]
    return before, after


def close_residual(acc_ref, near_ref, far_ref, s3_ref, p3_ref):
    width = s3_ref.shape[2]
    last = s3_ref.shape[1] - width
    before, after = sides_of(near_ref, far_ref, acc_ref.shape[0])
    first = acc_ref[:, :width] - times_split(before, *(s3_ref[j, :width, :] for j in range(3)))
    final = acc_ref[:, last:] - times_split(after, *(p3_ref[j, last:, :] for j in range(3)))
    return first, acc_ref[:, width:last], final


def squares(parts):
    total = None
    for part in parts:
        for i in range(0, part.shape[1], 128):
            piece = part[:, i : i + 128]
            total = piece * piece if total is None else total + piece * piece
    return total


def lane_row(total, turn, lanes):
    total = jnp.sum(total, axis=1, keepdims=True)
    rows = total.shape[0]
    row = lax.broadcasted_iota(jnp.int32, (rows, lanes), 0)
    lane = lax.broadcasted_iota(jnp.int32, (rows, lanes), 1)
    return jnp.sum(jnp.where(lane == row + turn * rows, total, 0.0), axis=0, keepdims=True)


def solve_kernel(acc_ref, near_ref, far_ref, s3_ref, p3_ref, z_ref, mix_ref, both_ref, top_ref, local_ref, norm_ref):
    parts = close_residual(acc_ref, near_ref, far_ref, s3_ref, p3_ref)
    width = s3_ref.shape[2]
    rows = acc_ref.shape[0]
    rounded = jnp.concatenate([p.astype(BF16) for p in parts], 1)
    local = dot(rounded, z_ref[...])
    local_ref[...] = local
    own_top = local[:, :width]
    mixed = times_split(split3(own_top), *(mix_ref[j] for j in range(3)))
    both_ref[:rows, :] = local[:, -width:] - mixed
    both_ref[rows:, :] = own_top
    top_ref[...] = own_top
    norm_ref[...] = squares(parts)


def norm_kernel(acc_ref, near_ref, far_ref, s3_ref, p3_ref, middle_ref, rest_ref, norm_ref, *, turn):
    first, _, final = close_residual(acc_ref, near_ref, far_ref, s3_ref, p3_ref)
    row = rest_ref[...] + lane_row(middle_ref[...] + squares((first, final)), turn, norm_ref.shape[1])
    norm_ref[...] = jnp.broadcast_to(row, norm_ref.shape)


def mix_kernel(near_ref, far_ref, chain_ref, before_ref, after_ref, mix_ref):
    even = is_even()
    width = chain_ref.shape[0]
    spikes = pl.ds(far_ref.shape[0] - width, width)
    near, far = near_ref[spikes, :], far_ref[spikes, :]
    before = choose(even, far, near)
    before_ref[...] = before
    after_ref[...] = choose(even, near, far)
    for j, part in enumerate(split3(dot(before, chain_ref[...]))):
        mix_ref[j] = part


def pair_kernel(own_ref, near_ref, second_ref, prefix_ref, whole_ref):
    right = on_right(0)
    width = own_ref.shape[0]
    own = own_ref[...].astype(F32)
    other = near_ref[pl.ds(near_ref.shape[0] - width, width), :].astype(F32)
    second = jnp.where(right, own, other).astype(BF16)
    first = jnp.where(right, other, own).astype(BF16)
    second_ref[...] = second
    row = lax.broadcasted_iota(jnp.int32, (width, width), 0)
    col = lax.broadcasted_iota(jnp.int32, (width, width), 1)
    prefix = jnp.where(right, other, jnp.where(row == col, 1.0, 0.0))
    for j, part in enumerate(split3(prefix)):
        prefix_ref[j] = part
    whole_ref[...] = dot(first, second)


def next_level(level, whole, other, prefix, second_ref, prefix_out, whole_out=None, half_out=None):
    right = on_right(level)
    second3 = split3(jnp.where(right, whole, other))
    first3 = split3(jnp.where(right, other, whole))
    for j, part in enumerate(second3):
        second_ref[j] = part
    product = None
    if whole_out is not None:
        product = times_split(first3, *second3)
        whole_out[...] = product
        if half_out is not None:
            half = half_out.shape[0]
            half_out[...] = jnp.where(is_even(), product[:half], product[half:])
    for j, part in enumerate(split3(times_split(first3, *prefix))):
        prefix_out[j] = choose(right, part, prefix[j])
    return product


def static_kernel(whole_ref, got_ref, twin_ref, prefix_ref, *outs, level):
    even = is_even()
    got, twin = got_ref[...], twin_ref[...]
    other = jnp.concatenate([jnp.where(even, twin, got), jnp.where(even, got, twin)], 0)
    next_level(level, whole_ref[...], other, parts_of(prefix_ref), *outs)


def chip_kernel(whole_ref, got_ref, twin_ref, prefix_ref, *outs):
    even = is_even()
    got, twin = got_ref[...], twin_ref[...]
    other = dot(choose(even, twin, got), choose(even, got, twin))
    next_level(1, whole_ref[...], other, parts_of(prefix_ref), *outs)


def merged(right, total, got, matrix):
    first = split3(jnp.where(right, got, total))
    product = times_split(first, *matrix) if isinstance(matrix, list) else times_exact(first, matrix)
    return product + jnp.where(right, total, got)


def parts_of(ref):
    return [ref[j] for j in range(3)]


def carry_step(level, values, reach_ref):
    return jnp.where(on_right(level), times_split(split3(values), *parts_of(reach_ref)), 0.0)


def sent_on(level, total, second_ref, carried_ref):
    product = times_split(split3(total), *parts_of(second_ref))
    carried_ref[...] = jnp.where(on_right(level), total, product)


def level0_kernel(both_ref, got_ref, second_ref, total_ref, carry_ref):
    right = on_right(0)
    rows = total_ref.shape[0]
    total, got = both_ref[:rows, :], got_ref[:rows, :]
    carry_ref[...] = jnp.where(right, got, 0.0)
    total_ref[...] = merged(right, total, got, second_ref[...])


def level0_wide_kernel(both_ref, got_ref, second_ref, next_ref, total_ref, carry_ref, carried_ref):
    level0_kernel(both_ref, got_ref, second_ref, total_ref, carry_ref)
    sent_on(1, total_ref[...], next_ref, carried_ref)


def level_kernel(total_ref, got_ref, carry_ref, reach_ref, second_ref, total_out, carry_out, *, level):
    got = got_ref[...]
    total_out[...] = merged(on_right(level), total_ref[...], got, parts_of(second_ref))
    carry_out[...] = carry_ref[...] + carry_step(level, got, reach_ref)


def wide_kernel(
    total_ref, carried_ref, got_ref, low_ref, cross_ref, carry_ref, reach_ref, reach2_ref, second_ref, second2_ref,
    *rest, level
):
    next_ref = rest[0] if len(rest) == 4 else None
    total_out, carry_out = rest[-3:-1] if next_ref is not None else rest
    right, right2 = on_right(level), on_right(level + 1)
    got, low = got_ref[...], low_ref[...] + cross_ref[...]
    carry_out[...] = carry_ref[...] + carry_step(level, got, reach_ref) + carry_step(level + 1, low, reach2_ref)
    passed = times_split(split3(got), *parts_of(second_ref))
    pair = jnp.where(right, passed + total_ref[...], carried_ref[...] + got)
    total = merged(right2, pair, low, parts_of(second2_ref))
    total_out[...] = total
    if next_ref is not None:
        sent_on(level + 2, total, next_ref, rest[-1])


def tips_kernel(*refs, level, wide):
    gots, refs = refs[: 3 if wide else 1], refs[3 if wide else 1 :]
    reaches, refs = refs[: 2 if wide else 1], refs[2 if wide else 1 :]
    carry_ref, near_ref, far_ref, local_ref, x_ref, u_ref, l_ref, before_ref, after_ref, chain_ref = refs[:10]
    top_out, previous_out, near_out, far_out = refs[10:]
    even = is_even()
    rows, width = carry_ref.shape
    carry = carry_ref[...] + carry_step(level, gots[0][...], reaches[0])
    if wide:
        carry = carry + carry_step(level + 1, gots[1][...] + gots[2][...], reaches[1])
    own_top = local_ref[:, :width]
    own_bottom = local_ref[:, -width:]
    next_top = jnp.where(even, near_ref[rows:, :], far_ref[...])
    offset = own_bottom - times_exact(split3(next_top), u_ref[:, -width:])
    previous = carry - times_exact(split3(own_top), before_ref[...])
    bottom = offset + times_exact(split3(previous), chain_ref[...])
    top = (next_top - times_exact(split3(bottom), after_ref[...])).astype(BF16)
    previous = previous.astype(BF16)
    top_out[...] = top
    previous_out[...] = previous

    def updated(columns):
        change = local_ref[:, columns] - dot(top, u_ref[:, columns]) - dot(previous, l_ref[:, columns])
        return x_ref[:, columns] + change

    size = x_ref.shape[1]
    first = updated(slice(0, width))
    final = updated(slice(size - width, size))
    near_out[...] = jnp.where(even, final, first)
    far_out[...] = jnp.where(even, first, final)


def update_kernel(top_ref, previous_ref, local_ref, x_ref, u_ref, l_ref, b_ref, d3_ref, s3_ref, p3_ref, *refs):
    x_out, acc_ref = refs[-2:] if len(refs) == 2 else refs[-4:-2]
    change = local_ref[...] - dot(top_ref[...], u_ref[...]) - dot(previous_ref[...], l_ref[...])
    x_out[...] = x_ref[...] + change
    local_part(b_ref, x_out, d3_ref, s3_ref, p3_ref, acc_ref)
    if len(refs) > 2:
        norms, middle_ref, row_ref = refs[:-4], refs[-2], refs[-1]
        width = d3_ref.shape[2]
        middle_ref[...] = squares((acc_ref[:, width : acc_ref.shape[1] - width],))
        row_ref[...] = sum(lane_row(ref[...], turn, row_ref.shape[1]) for turn, ref in enumerate(norms))


def finish_kernel(gathered_ref, out_ref, *, total):
    sums = jnp.sqrt(jnp.sum(gathered_ref[...], axis=0, keepdims=True) / total)
    rows = out_ref.shape[1]
    for turn in range(out_ref.shape[0]):
        out_ref[pl.ds(turn, 1), :] = sums[:, turn * rows : (turn + 1) * rows]


def body(
    right_sides,
    initial,
    diag_blocks,
    sub_blocks,
    super_blocks,
    local_inverse,
    upper_spikes,
    lower_spikes,
):
    width = diag_blocks.shape[1]
    rows, size = right_sides.shape
    count = lax.axis_size(AXIS)
    levels = (count - 1).bit_length()
    tip = ((rows, width), F32)
    low_tip = ((rows, width), BF16)
    square = ((width, width), F32)
    low_square = ((width, width), BF16)
    triple = ((3, width, width), BF16)
    half = ((width // 2, width), F32)
    wide = ((rows, size), F32)
    big = ((3, size, width), BF16)
    lanes = -(-rows * (ITERS + 1) // 128) * 128

    near_pack, far_pack, chain = kernel_call(
        payload_kernel,
        [((3 * rows + 2 * width, width), BF16), ((3 * rows + width, width), BF16), low_square],
        (initial,), (upper_spikes,), (lower_spikes,),
    )
    near = exchange(near_pack, 1)
    far = across(far_pack)
    acc, right_sides, solution, d3, s3, p3, local_inverse, upper_spikes, lower_spikes = kernel_call(
        first_local_kernel,
        [wide, wide, wide, big, big, big, (local_inverse.shape, BF16), (upper_spikes.shape, BF16), (lower_spikes.shape, BF16)],
        *((a,) for a in (right_sides, initial, diag_blocks, sub_blocks, super_blocks, local_inverse, upper_spikes, lower_spikes)),
        micros=3,
    )
    before, after, mix = kernel_call(mix_kernel, [low_square, low_square, triple], near, far, chain)

    def swap(values, distance):
        return exchange(values, distance | 1)

    second, prefix, whole = kernel_call(pair_kernel, [low_square, triple, square], chain, near)
    seconds, reaches = [second], [None, prefix]
    for level in range(1, levels - 1):
        got = swap(chain if level == 1 else piece, 1 << level)
        twin = swap(got, 1)
        kernel = chip_kernel if level == 1 else functools.partial(static_kernel, level=level)
        second, prefix, *rest = kernel_call(
            kernel, [triple, triple] + [square, half] * (level < levels - 2), whole, got, twin, prefix, micros=1
        )
        if rest:
            whole, piece = rest
        seconds.append(second)
        reaches.append(prefix)

    norms = []
    for turn in range(ITERS):
        both, own_top, local, norm = kernel_call(
            solve_kernel, [((2 * rows, width), F32), tip, wide, ((rows, 128), F32)],
            acc, near, far, s3, p3, local_inverse, mix, micros=0.8,
        )
        norms.append(norm)
        swapped = swap(both, 1)
        far_top = across(own_top)
        groups = [(0, 1)]
        while sum(groups[-1]) < levels:
            level = sum(groups[-1])
            groups.append((level, 2 if turn > 0 and level + 2 <= levels else 1))
        carried = None
        for i, (level, size_of) in enumerate(groups[:-1]):
            after_size = groups[i + 1][1]
            outs = [tip, tip] + [tip] * (after_size == 2)
            following = [seconds[level + size_of]] if after_size == 2 else []
            if level == 0:
                kernel = level0_wide_kernel if after_size == 2 else level0_kernel
                total, carry, *more = kernel_call(kernel, outs, both, swapped, seconds[0], *following)
            elif size_of == 1:
                got = swap(total, 1 << level)
                total, carry, *more = kernel_call(
                    functools.partial(level_kernel, level=level), outs, total, got, carry, reaches[level], seconds[level]
                )
            else:
                step = 1 << level
                got = swap(total, step)
                low = swap(carried, 2 * step)
                cross = swap(carried, 3 * step)
                total, carry, *more = kernel_call(
                    functools.partial(wide_kernel, level=level), outs, total, carried, got, low, cross, carry,
                    reaches[level], reaches[level + 1], seconds[level], seconds[level + 1], *following,
                )
            carried = more[0] if more else None
        level, size_of = groups[-1]
        gots = [swap(total, 1 << level)]
        if size_of == 2:
            gots.append(swap(carried, 2 << level))
            gots.append(swap(carried, 3 << level))
        top, previous, near, far = kernel_call(
            functools.partial(tips_kernel, level=level, wide=size_of == 2), [low_tip, low_tip, tip, tip],
            *gots, *reaches[level : level + size_of], carry, swapped, far_top, local, solution, upper_spikes, lower_spikes,
            before, after, chain, micros=1,
        )
        near = exchange(near, 1)
        far = across(far)
        final = turn == ITERS - 1
        solution, acc, *sums = kernel_call(
            update_kernel, [wide, wide] + [((rows, 128), F32), ((1, lanes), F32)] * final,
            top, previous, local, solution, upper_spikes, lower_spikes, right_sides, d3, s3, p3, *(norms if final else ()),
            micros=1,
        )
    mine = kernel_call(
        functools.partial(norm_kernel, turn=ITERS), [((count, lanes), F32)], acc, near, far, s3, p3, *sums
    )[0]
    gathered = lax.all_to_all(mine, AXIS, 0, 0, tiled=True)
    result = pl.pallas_call(
        functools.partial(finish_kernel, total=size * count), out_shape=jax.ShapeDtypeStruct((ITERS + 1, rows), F32),
        compiler_params=pltpu.CompilerParams(vmem_limit_bytes=16 * 2**20),
    )(gathered)
    return solution, result


def solution(mesh):
    return jax.shard_map(
        body,
        mesh=mesh,
        in_specs=(
            P(None, AXIS),
            P(None, AXIS),
            P(AXIS, None),
            P(AXIS, None),
            P(AXIS, None),
            P(AXIS, None),
            P(None, AXIS),
            P(None, AXIS),
        ),
        out_specs=(P(None, AXIS), P()),
        check_vma=False,
    )
```

```python
import functools
import math

import jax
import jax.numpy as jnp
from jax import lax
from jax.experimental import pallas as pl
from jax.experimental.pallas import tpu as pltpu
from jax.sharding import PartitionSpec as P


ITERS = 2
AXIS = "rows"
F32 = jnp.float32
BF16 = jnp.bfloat16


def exchange(values, distance):
    count = lax.axis_size(AXIS)
    return lax.ppermute(values, AXIS, [(i, i ^ distance) for i in range(count)])


def across(values):
    count = lax.axis_size(AXIS)
    pairs = [(i, i + 1) for i in range(1, count - 1, 2)]
    return lax.ppermute(values, AXIS, pairs + [(b, a) for a, b in pairs])


def kernel_call(kernel, outs, *args, micros=0.3):
    specs = [
        pl.BlockSpec(memory_space=pltpu.HBM if isinstance(a, tuple) else pltpu.VMEM) for a in args
    ]
    held = sum(math.prod(shape) * jnp.dtype(dtype).itemsize for shape, dtype in outs)
    return pl.pallas_call(
        kernel,
        in_specs=specs,
        out_specs=[pl.BlockSpec(memory_space=pltpu.VMEM)] * len(outs),
        out_shape=[pltpu.VMEM(shape, dtype) for shape, dtype in outs],
        scratch_shapes=[],
        cost_estimate=pl.CostEstimate(flops=int(micros * 1e8), transcendentals=0, bytes_accessed=held),
        compiler_params=pltpu.CompilerParams(vmem_limit_bytes=16 * 2**20),
    )(*(pltpu.with_memory_space_constraint(a[0], pltpu.HBM) if isinstance(a, tuple) else a for a in args))


def is_even():
    return lax.axis_index(AXIS) % 2 == 0


def on_right(level):
    return (lax.axis_index(AXIS) >> level) % 2 == 1


def split3(values):
    high = values.astype(BF16)
    rest = values - high.astype(F32)
    mid = rest.astype(BF16)
    low = (rest - mid.astype(F32)).astype(BF16)
    return high, mid, low


def dot(left, right):
    return jnp.dot(left, right, preferred_element_type=F32)


def fold(product, count):
    rows = product.shape[0] // count
    total = product[(count - 1) * rows :]
    for i in range(count - 2, -1, -1):
        total = total + product[i * rows : (i + 1) * rows]
    return total


def times_exact(parts, right):
    return fold(dot(jnp.concatenate(parts, 0), right), 3)


def times_split(parts, high, mid, low):
    small = dot(parts[0], low) + fold(dot(jnp.concatenate(parts[:2], 0), mid), 2)
    return fold(dot(jnp.concatenate(parts, 0), high), 3) + small


def gather_copies(pairs, sems):
    copies = [pltpu.make_async_copy(a, b, sems.at[i]) for i, (a, b) in enumerate(pairs)]
    for copy in copies:
        copy.start()
    return copies


def payload_kernel(x_hbm, u_hbm, l_hbm, near_ref, far_ref, chain_ref):
    even = is_even()
    width = chain_ref.shape[0]
    rows = x_hbm.shape[0]
    last = x_hbm.shape[1] - width

    def work(first, final, up, low, bottom, sems):
        head, tail = pl.ds(0, width), pl.ds(last, width)
        copies = gather_copies(
            [
                (x_hbm.at[:, head], first),
                (x_hbm.at[:, tail], final),
                (l_hbm.at[:, tail], bottom),
                (u_hbm.at[:, tail], up),
                (l_hbm.at[:, head], low),
            ],
            sems,
        )
        for copy in copies:
            copy.wait()
        for ref, here, there in ((near_ref, final, first), (far_ref, first, final)):
            for j, part in enumerate(split3(jnp.where(even, here[...], there[...]))):
                ref[pl.ds(j * rows, rows), :] = part
        chain = -bottom[...]
        chain_ref[...] = chain
        low_tip, up_tip = low[...].astype(F32), up[...].astype(F32)
        near_ref[pl.ds(3 * rows, width), :] = jnp.where(even, up_tip, low_tip).astype(BF16)
        far_ref[pl.ds(3 * rows, width), :] = jnp.where(even, low_tip, up_tip).astype(BF16)
        near_ref[pl.ds(3 * rows + width, width), :] = chain

    vec = pltpu.VMEM((rows, width), F32)
    mat = pltpu.VMEM(chain_ref.shape, BF16)
    pl.run_scoped(work, vec, vec, mat, mat, mat, pltpu.SemaphoreType.DMA((5,)))


def split_store(ref, rows, values):
    for j, part in enumerate(split3(values)):
        ref[j, rows, :] = part


def first_local_kernel(b_hbm, x_hbm, d_hbm, s_hbm, p_hbm, z_hbm, u_hbm, l_hbm, acc_ref, b_ref, x_ref, d3_ref, s3_ref, p3_ref, z_ref, u_ref, l_ref):
    width = d_hbm.shape[1]

    def work(d_ref, s_ref, p_ref, sems):
        copies = gather_copies(
            [(x_hbm, x_ref), (d_hbm, d_ref), (s_hbm, s_ref), (p_hbm, p_ref), (b_hbm, b_ref), (z_hbm, z_ref), (u_hbm, u_ref), (l_hbm, l_ref)],
            sems,
        )
        for copy in copies[:2]:
            copy.wait()
        for source, target, copy in ((d_ref, d3_ref, 2), (s_ref, s3_ref, 3), (p_ref, p3_ref, 4)):
            for k in range(d_ref.shape[0] // width):
                split_store(target, pl.ds(k * width, width), source[k * width : (k + 1) * width, :])
            copies[copy].wait()
        local_part(b_ref, x_ref, d3_ref, s3_ref, p3_ref, acc_ref)
        for copy in copies[5:]:
            copy.wait()

    mat = pltpu.VMEM(d_hbm.shape, F32)
    pl.run_scoped(work, mat, mat, mat, pltpu.SemaphoreType.DMA((8,)))


def local_part(b_ref, x_ref, d3_ref, s3_ref, p3_ref, acc_ref):
    width = d3_ref.shape[2]
    last = d3_ref.shape[1] // width - 1
    x = [split3(x_ref[:, k * width : (k + 1) * width]) for k in range(last + 1)]
    for k in range(last + 1):
        rows = pl.ds(k * width, width)
        part = times_split(x[k], *(d3_ref[j, rows, :] for j in range(3)))
        if k > 0:
            part = part + times_split(x[k - 1], *(s3_ref[j, rows, :] for j in range(3)))
        if k < last:
            part = part + times_split(x[k + 1], *(p3_ref[j, rows, :] for j in range(3)))
        acc_ref[:, k * width : (k + 1) * width] = b_ref[:, k * width : (k + 1) * width] - part


def choose(condition, left, right):
    return jnp.where(condition, left.astype(F32), right.astype(F32)).astype(left.dtype)


def sides_of(near_ref, far_ref, rows):
    even = is_even()
    if near_ref.dtype == F32:
        near, far = near_ref[...], far_ref[...]
        return split3(jnp.where(even, far, near)), split3(jnp.where(even, near, far))
    near = [near_ref[pl.ds(j * rows, rows), :] for j in range(3)]
    far = [far_ref[pl.ds(j * rows, rows), :] for j in range(3)]
    before = [choose(even, f, n) for n, f in zip(near, far)]
    after = [choose(even, n, f) for n, f in zip(near, far)]
    return before, after


def close_residual(acc_ref, near_ref, far_ref, s3_ref, p3_ref):
    width = s3_ref.shape[2]
    last = s3_ref.shape[1] - width
    before, after = sides_of(near_ref, far_ref, acc_ref.shape[0])
    first = acc_ref[:, :width] - times_split(before, *(s3_ref[j, :width, :] for j in range(3)))
    final = acc_ref[:, last:] - times_split(after, *(p3_ref[j, last:, :] for j in range(3)))
    return first, acc_ref[:, width:last], final


def squares(parts):
    total = None
    for part in parts:
        for i in range(0, part.shape[1], 128):
            piece = part[:, i : i + 128]
            total = piece * piece if total is None else total + piece * piece
    return total


def lane_row(total, turn, lanes):
    total = jnp.sum(total, axis=1, keepdims=True)
    rows = total.shape[0]
    row = lax.broadcasted_iota(jnp.int32, (rows, lanes), 0)
    lane = lax.broadcasted_iota(jnp.int32, (rows, lanes), 1)
    return jnp.sum(jnp.where(lane == row + turn * rows, total, 0.0), axis=0, keepdims=True)


def solve_kernel(acc_ref, near_ref, far_ref, s3_ref, p3_ref, z_ref, mix_ref, both_ref, top_ref, local_ref, norm_ref):
    parts = close_residual(acc_ref, near_ref, far_ref, s3_ref, p3_ref)
    width = s3_ref.shape[2]
    rows = acc_ref.shape[0]
    rounded = jnp.concatenate([p.astype(BF16) for p in parts], 1)
    local = dot(rounded, z_ref[...])
    local_ref[...] = local
    own_top = local[:, :width]
    mixed = times_split(split3(own_top), *(mix_ref[j] for j in range(3)))
    both_ref[:rows, :] = local[:, -width:] - mixed
    both_ref[rows:, :] = own_top
    top_ref[...] = own_top
    norm_ref[...] = squares(parts)


def norm_kernel(acc_ref, near_ref, far_ref, s3_ref, p3_ref, middle_ref, rest_ref, norm_ref, *, turn):
    first, _, final = close_residual(acc_ref, near_ref, far_ref, s3_ref, p3_ref)
    row = rest_ref[...] + lane_row(middle_ref[...] + squares((first, final)), turn, norm_ref.shape[1])
    norm_ref[...] = jnp.broadcast_to(row, norm_ref.shape)


def mix_kernel(near_ref, far_ref, chain_ref, before_ref, after_ref, mix_ref):
    even = is_even()
    width = chain_ref.shape[0]
    spikes = pl.ds(far_ref.shape[0] - width, width)
    near, far = near_ref[spikes, :], far_ref[spikes, :]
    before = choose(even, far, near)
    before_ref[...] = before
    after_ref[...] = choose(even, near, far)
    for j, part in enumerate(split3(dot(before, chain_ref[...]))):
        mix_ref[j] = part


def pair_kernel(own_ref, near_ref, second_ref, prefix_ref, whole_ref):
    right = on_right(0)
    width = own_ref.shape[0]
    own = own_ref[...].astype(F32)
    other = near_ref[pl.ds(near_ref.shape[0] - width, width), :].astype(F32)
    second = jnp.where(right, own, other).astype(BF16)
    first = jnp.where(right, other, own).astype(BF16)
    second_ref[...] = second
    row = lax.broadcasted_iota(jnp.int32, (width, width), 0)
    col = lax.broadcasted_iota(jnp.int32, (width, width), 1)
    prefix = jnp.where(right, other, jnp.where(row == col, 1.0, 0.0))
    for j, part in enumerate(split3(prefix)):
        prefix_ref[j] = part
    whole_ref[...] = dot(first, second)


def next_level(level, whole, other, prefix, second_ref, prefix_out, whole_out=None, half_out=None):
    right = on_right(level)
    second3 = split3(jnp.where(right, whole, other))
    first3 = split3(jnp.where(right, other, whole))
    for j, part in enumerate(second3):
        second_ref[j] = part
    product = None
    if whole_out is not None:
        product = times_split(first3, *second3)
        whole_out[...] = product
        if half_out is not None:
            half = half_out.shape[0]
            half_out[...] = jnp.where(is_even(), product[:half], product[half:])
    for j, part in enumerate(split3(times_split(first3, *prefix))):
        prefix_out[j] = choose(right, part, prefix[j])
    return product


def static_kernel(whole_ref, got_ref, twin_ref, prefix_ref, *outs, level):
    even = is_even()
    got, twin = got_ref[...], twin_ref[...]
    other = jnp.concatenate([jnp.where(even, twin, got), jnp.where(even, got, twin)], 0)
    next_level(level, whole_ref[...], other, parts_of(prefix_ref), *outs)


def chip_kernel(whole_ref, got_ref, twin_ref, prefix_ref, *outs):
    even = is_even()
    got, twin = got_ref[...], twin_ref[...]
    other = dot(choose(even, twin, got), choose(even, got, twin))
    next_level(1, whole_ref[...], other, parts_of(prefix_ref), *outs)


def merged(right, total, got, matrix):
    first = split3(jnp.where(right, got, total))
    product = times_split(first, *matrix) if isinstance(matrix, list) else times_exact(first, matrix)
    return product + jnp.where(right, total, got)


def parts_of(ref):
    return [ref[j] for j in range(3)]


def carry_step(level, values, reach_ref):
    return jnp.where(on_right(level), times_split(split3(values), *parts_of(reach_ref)), 0.0)


def sent_on(level, total, second_ref, carried_ref):
    product = times_split(split3(total), *parts_of(second_ref))
    carried_ref[...] = jnp.where(on_right(level), total, product)


def level0_kernel(both_ref, got_ref, second_ref, total_ref, carry_ref):
    right = on_right(0)
    rows = total_ref.shape[0]
    total, got = both_ref[:rows, :], got_ref[:rows, :]
    carry_ref[...] = jnp.where(right, got, 0.0)
    total_ref[...] = merged(right, total, got, second_ref[...])


def level0_wide_kernel(both_ref, got_ref, second_ref, next_ref, total_ref, carry_ref, carried_ref):
    level0_kernel(both_ref, got_ref, second_ref, total_ref, carry_ref)
    sent_on(1, total_ref[...], next_ref, carried_ref)


def level_kernel(total_ref, got_ref, carry_ref, reach_ref, second_ref, total_out, carry_out, *, level):
    got = got_ref[...]
    total_out[...] = merged(on_right(level), total_ref[...], got, parts_of(second_ref))
    carry_out[...] = carry_ref[...] + carry_step(level, got, reach_ref)


def wide_kernel(
    total_ref, carried_ref, got_ref, low_ref, cross_ref, carry_ref, reach_ref, reach2_ref, second_ref, second2_ref,
    *rest, level
):
    next_ref = rest[0] if len(rest) == 4 else None
    total_out, carry_out = rest[-3:-1] if next_ref is not None else rest
    right, right2 = on_right(level), on_right(level + 1)
    got, low = got_ref[...], low_ref[...] + cross_ref[...]
    carry_out[...] = carry_ref[...] + carry_step(level, got, reach_ref) + carry_step(level + 1, low, reach2_ref)
    passed = times_split(split3(got), *parts_of(second_ref))
    pair = jnp.where(right, passed + total_ref[...], carried_ref[...] + got)
    total = merged(right2, pair, low, parts_of(second2_ref))
    total_out[...] = total
    if next_ref is not None:
        sent_on(level + 2, total, next_ref, rest[-1])


def tips_kernel(*refs, level, wide):
    gots, refs = refs[: 3 if wide else 1], refs[3 if wide else 1 :]
    reaches, refs = refs[: 2 if wide else 1], refs[2 if wide else 1 :]
    carry_ref, near_ref, far_ref, local_ref, x_ref, u_ref, l_ref, before_ref, after_ref, chain_ref = refs[:10]
    top_out, previous_out, near_out, far_out = refs[10:]
    even = is_even()
    rows, width = carry_ref.shape
    carry = carry_ref[...] + carry_step(level, gots[0][...], reaches[0])
    if wide:
        carry = carry + carry_step(level + 1, gots[1][...] + gots[2][...], reaches[1])
    own_top = local_ref[:, :width]
    own_bottom = local_ref[:, -width:]
    next_top = jnp.where(even, near_ref[rows:, :], far_ref[...])
    offset = own_bottom - times_exact(split3(next_top), u_ref[:, -width:])
    previous = carry - times_exact(split3(own_top), before_ref[...])
    bottom = offset + times_exact(split3(previous), chain_ref[...])
    top = (next_top - times_exact(split3(bottom), after_ref[...])).astype(BF16)
    previous = previous.astype(BF16)
    top_out[...] = top
    previous_out[...] = previous

    def updated(columns):
        change = local_ref[:, columns] - dot(top, u_ref[:, columns]) - dot(previous, l_ref[:, columns])
        return x_ref[:, columns] + change

    size = x_ref.shape[1]
    first = updated(slice(0, width))
    final = updated(slice(size - width, size))
    near_out[...] = jnp.where(even, final, first)
    far_out[...] = jnp.where(even, first, final)


def update_kernel(top_ref, previous_ref, local_ref, x_ref, u_ref, l_ref, b_ref, d3_ref, s3_ref, p3_ref, *refs):
    x_out, acc_ref = refs[-2:] if len(refs) == 2 else refs[-4:-2]
    change = local_ref[...] - dot(top_ref[...], u_ref[...]) - dot(previous_ref[...], l_ref[...])
    x_out[...] = x_ref[...] + change
    local_part(b_ref, x_out, d3_ref, s3_ref, p3_ref, acc_ref)
    if len(refs) > 2:
        norms, middle_ref, row_ref = refs[:-4], refs[-2], refs[-1]
        width = d3_ref.shape[2]
        middle_ref[...] = squares((acc_ref[:, width : acc_ref.shape[1] - width],))
        row_ref[...] = sum(lane_row(ref[...], turn, row_ref.shape[1]) for turn, ref in enumerate(norms))


def finish_kernel(gathered_ref, out_ref, *, total):
    sums = jnp.sqrt(jnp.sum(gathered_ref[...], axis=0, keepdims=True) / total)
    rows = out_ref.shape[1]
    for turn in range(out_ref.shape[0]):
        out_ref[pl.ds(turn, 1), :] = sums[:, turn * rows : (turn + 1) * rows]


def body(
    right_sides,
    initial,
    diag_blocks,
    sub_blocks,
    super_blocks,
    local_inverse,
    upper_spikes,
    lower_spikes,
):
    width = diag_blocks.shape[1]
    rows, size = right_sides.shape
    count = lax.axis_size(AXIS)
    levels = (count - 1).bit_length()
    tip = ((rows, width), F32)
    low_tip = ((rows, width), BF16)
    square = ((width, width), F32)
    low_square = ((width, width), BF16)
    triple = ((3, width, width), BF16)
    half = ((width // 2, width), F32)
    wide = ((rows, size), F32)
    big = ((3, size, width), BF16)
    lanes = -(-rows * (ITERS + 1) // 128) * 128

    near_pack, far_pack, chain = kernel_call(
        payload_kernel,
        [((3 * rows + 2 * width, width), BF16), ((3 * rows + width, width), BF16), low_square],
        (initial,), (upper_spikes,), (lower_spikes,),
    )
    near = exchange(near_pack, 1)
    far = across(far_pack)
    acc, right_sides, solution, d3, s3, p3, local_inverse, upper_spikes, lower_spikes = kernel_call(
        first_local_kernel,
        [wide, wide, wide, big, big, big, (local_inverse.shape, BF16), (upper_spikes.shape, BF16), (lower_spikes.shape, BF16)],
        *((a,) for a in (right_sides, initial, diag_blocks, sub_blocks, super_blocks, local_inverse, upper_spikes, lower_spikes)),
        micros=3,
    )
    before, after, mix = kernel_call(mix_kernel, [low_square, low_square, triple], near, far, chain)

    def swap(values, distance):
        return exchange(values, distance | 1)

    second, prefix, whole = kernel_call(pair_kernel, [low_square, triple, square], chain, near)
    seconds, reaches = [second], [None, prefix]
    for level in range(1, levels - 1):
        got = swap(chain if level == 1 else piece, 1 << level)
        twin = swap(got, 1)
        kernel = chip_kernel if level == 1 else functools.partial(static_kernel, level=level)
        second, prefix, *rest = kernel_call(
            kernel, [triple, triple] + [square, half] * (level < levels - 2), whole, got, twin, prefix, micros=1
        )
        if rest:
            whole, piece = rest
        seconds.append(second)
        reaches.append(prefix)

    norms = []
    for turn in range(ITERS):
        both, own_top, local, norm = kernel_call(
            solve_kernel, [((2 * rows, width), F32), tip, wide, ((rows, 128), F32)],
            acc, near, far, s3, p3, local_inverse, mix, micros=0.8,
        )
        norms.append(norm)
        swapped = swap(both, 1)
        far_top = across(own_top)
        groups = [(0, 1)]
        while sum(groups[-1]) < levels:
            level = sum(groups[-1])
            groups.append((level, 2 if (turn > 0 or level == 1) and level + 2 <= levels else 1))
        carried = None
        for i, (level, size_of) in enumerate(groups[:-1]):
            after_size = groups[i + 1][1]
            outs = [tip, tip] + [tip] * (after_size == 2)
            following = [seconds[level + size_of]] if after_size == 2 else []
            if level == 0:
                kernel = level0_wide_kernel if after_size == 2 else level0_kernel
                total, carry, *more = kernel_call(kernel, outs, both, swapped, seconds[0], *following)
            elif size_of == 1:
                got = swap(total, 1 << level)
                total, carry, *more = kernel_call(
                    functools.partial(level_kernel, level=level), outs, total, got, carry, reaches[level], seconds[level]
                )
            else:
                step = 1 << level
                got = swap(total, step)
                low = swap(carried, 2 * step)
                cross = swap(carried, 3 * step)
                total, carry, *more = kernel_call(
                    functools.partial(wide_kernel, level=level), outs, total, carried, got, low, cross, carry,
                    reaches[level], reaches[level + 1], seconds[level], seconds[level + 1], *following,
                )
            carried = more[0] if more else None
        level, size_of = groups[-1]
        gots = [swap(total, 1 << level)]
        if size_of == 2:
            gots.append(swap(carried, 2 << level))
            gots.append(swap(carried, 3 << level))
        top, previous, near, far = kernel_call(
            functools.partial(tips_kernel, level=level, wide=size_of == 2), [low_tip, low_tip, tip, tip],
            *gots, *reaches[level : level + size_of], carry, swapped, far_top, local, solution, upper_spikes, lower_spikes,
            before, after, chain, micros=1,
        )
        near = exchange(near, 1)
        far = across(far)
        final = turn == ITERS - 1
        solution, acc, *sums = kernel_call(
            update_kernel, [wide, wide] + [((rows, 128), F32), ((1, lanes), F32)] * final,
            top, previous, local, solution, upper_spikes, lower_spikes, right_sides, d3, s3, p3, *(norms if final else ()),
            micros=1,
        )
    mine = kernel_call(
        functools.partial(norm_kernel, turn=ITERS), [((count, lanes), F32)], acc, near, far, s3, p3, *sums
    )[0]
    gathered = lax.all_to_all(mine, AXIS, 0, 0, tiled=True)
    result = pl.pallas_call(
        functools.partial(finish_kernel, total=size * count), out_shape=jax.ShapeDtypeStruct((ITERS + 1, rows), F32),
        compiler_params=pltpu.CompilerParams(vmem_limit_bytes=16 * 2**20),
    )(gathered)
    return solution, result


def solution(mesh):
    return jax.shard_map(
        body,
        mesh=mesh,
        in_specs=(
            P(None, AXIS),
            P(None, AXIS),
            P(AXIS, None),
            P(AXIS, None),
            P(AXIS, None),
            P(AXIS, None),
            P(None, AXIS),
            P(None, AXIS),
        ),
        out_specs=(P(None, AXIS), P()),
        check_vma=False,
    )
```

```python
import functools
import math

import jax
import jax.numpy as jnp
from jax import lax
from jax.experimental import pallas as pl
from jax.experimental.pallas import tpu as pltpu
from jax.sharding import PartitionSpec as P


ITERS = 2
AXIS = "rows"
F32 = jnp.float32
BF16 = jnp.bfloat16


def exchange(values, distance):
    count = lax.axis_size(AXIS)
    return lax.ppermute(values, AXIS, [(i, i ^ distance) for i in range(count)])


def across(values):
    count = lax.axis_size(AXIS)
    pairs = [(i, i + 1) for i in range(1, count - 1, 2)]
    return lax.ppermute(values, AXIS, pairs + [(b, a) for a, b in pairs])


def kernel_call(kernel, outs, *args, micros=0.3):
    specs = [
        pl.BlockSpec(memory_space=pltpu.HBM if isinstance(a, tuple) else pltpu.VMEM) for a in args
    ]
    held = sum(math.prod(shape) * jnp.dtype(dtype).itemsize for shape, dtype in outs)
    return pl.pallas_call(
        kernel,
        in_specs=specs,
        out_specs=[pl.BlockSpec(memory_space=pltpu.VMEM)] * len(outs),
        out_shape=[pltpu.VMEM(shape, dtype) for shape, dtype in outs],
        scratch_shapes=[],
        cost_estimate=pl.CostEstimate(flops=int(micros * 1e8), transcendentals=0, bytes_accessed=held),
        compiler_params=pltpu.CompilerParams(vmem_limit_bytes=16 * 2**20),
    )(*(pltpu.with_memory_space_constraint(a[0], pltpu.HBM) if isinstance(a, tuple) else a for a in args))


def is_even():
    return lax.axis_index(AXIS) % 2 == 0


def on_right(level):
    return (lax.axis_index(AXIS) >> level) % 2 == 1


def split3(values):
    high = values.astype(BF16)
    rest = values - high.astype(F32)
    mid = rest.astype(BF16)
    low = (rest - mid.astype(F32)).astype(BF16)
    return high, mid, low


def dot(left, right):
    return jnp.dot(left, right, preferred_element_type=F32)


def fold(product, count):
    rows = product.shape[0] // count
    total = product[(count - 1) * rows :]
    for i in range(count - 2, -1, -1):
        total = total + product[i * rows : (i + 1) * rows]
    return total


def times_exact(parts, right):
    return fold(dot(jnp.concatenate(parts, 0), right), 3)


def times_split(parts, high, mid, low):
    small = dot(parts[0], low) + fold(dot(jnp.concatenate(parts[:2], 0), mid), 2)
    return fold(dot(jnp.concatenate(parts, 0), high), 3) + small


def gather_copies(pairs, sems):
    copies = [pltpu.make_async_copy(a, b, sems.at[i]) for i, (a, b) in enumerate(pairs)]
    for copy in copies:
        copy.start()
    return copies


def payload_kernel(x_hbm, u_hbm, l_hbm, near_ref, far_ref, chain_ref):
    even = is_even()
    width = chain_ref.shape[0]
    rows = x_hbm.shape[0]
    last = x_hbm.shape[1] - width

    def work(first, final, up, low, bottom, sems):
        head, tail = pl.ds(0, width), pl.ds(last, width)
        copies = gather_copies(
            [
                (x_hbm.at[:, head], first),
                (x_hbm.at[:, tail], final),
                (l_hbm.at[:, tail], bottom),
                (u_hbm.at[:, tail], up),
                (l_hbm.at[:, head], low),
            ],
            sems,
        )
        for copy in copies:
            copy.wait()
        for ref, here, there in ((near_ref, final, first), (far_ref, first, final)):
            for j, part in enumerate(split3(jnp.where(even, here[...], there[...]))):
                ref[pl.ds(j * rows, rows), :] = part
        chain = -bottom[...]
        chain_ref[...] = chain
        low_tip, up_tip = low[...].astype(F32), up[...].astype(F32)
        near_ref[pl.ds(3 * rows, width), :] = jnp.where(even, up_tip, low_tip).astype(BF16)
        far_ref[pl.ds(3 * rows, width), :] = jnp.where(even, low_tip, up_tip).astype(BF16)
        near_ref[pl.ds(3 * rows + width, width), :] = chain

    vec = pltpu.VMEM((rows, width), F32)
    mat = pltpu.VMEM(chain_ref.shape, BF16)
    pl.run_scoped(work, vec, vec, mat, mat, mat, pltpu.SemaphoreType.DMA((5,)))


def split_store(ref, rows, values):
    for j, part in enumerate(split3(values)):
        ref[j, rows, :] = part


def first_local_kernel(b_hbm, x_hbm, d_hbm, s_hbm, p_hbm, z_hbm, u_hbm, l_hbm, acc_ref, b_ref, x_ref, d3_ref, s3_ref, p3_ref, z_ref, u_ref, l_ref):
    width = d_hbm.shape[1]

    def work(d_ref, s_ref, p_ref, sems):
        copies = gather_copies(
            [(x_hbm, x_ref), (d_hbm, d_ref), (s_hbm, s_ref), (p_hbm, p_ref), (b_hbm, b_ref), (z_hbm, z_ref), (u_hbm, u_ref), (l_hbm, l_ref)],
            sems,
        )
        for copy in copies[:2]:
            copy.wait()
        for source, target, copy in ((d_ref, d3_ref, 2), (s_ref, s3_ref, 3), (p_ref, p3_ref, 4)):
            for k in range(d_ref.shape[0] // width):
                split_store(target, pl.ds(k * width, width), source[k * width : (k + 1) * width, :])
            copies[copy].wait()
        local_part(b_ref, x_ref, d3_ref, s3_ref, p3_ref, acc_ref)
        for copy in copies[5:]:
            copy.wait()

    mat = pltpu.VMEM(d_hbm.shape, F32)
    pl.run_scoped(work, mat, mat, mat, pltpu.SemaphoreType.DMA((8,)))


def local_part(b_ref, x_ref, d3_ref, s3_ref, p3_ref, acc_ref):
    width = d3_ref.shape[2]
    last = d3_ref.shape[1] // width - 1
    x = [split3(x_ref[:, k * width : (k + 1) * width]) for k in range(last + 1)]
    for k in range(last + 1):
        rows = pl.ds(k * width, width)
        part = times_split(x[k], *(d3_ref[j, rows, :] for j in range(3)))
        if k > 0:
            part = part + times_split(x[k - 1], *(s3_ref[j, rows, :] for j in range(3)))
        if k < last:
            part = part + times_split(x[k + 1], *(p3_ref[j, rows, :] for j in range(3)))
        acc_ref[:, k * width : (k + 1) * width] = b_ref[:, k * width : (k + 1) * width] - part


def choose(condition, left, right):
    return jnp.where(condition, left.astype(F32), right.astype(F32)).astype(left.dtype)


def sides_of(near_ref, far_ref, rows):
    even = is_even()
    if near_ref.dtype == F32:
        near, far = near_ref[...], far_ref[...]
        return split3(jnp.where(even, far, near)), split3(jnp.where(even, near, far))
    near = [near_ref[pl.ds(j * rows, rows), :] for j in range(3)]
    far = [far_ref[pl.ds(j * rows, rows), :] for j in range(3)]
    before = [choose(even, f, n) for n, f in zip(near, far)]
    after = [choose(even, n, f) for n, f in zip(near, far)]
    return before, after


def close_residual(acc_ref, near_ref, far_ref, s3_ref, p3_ref):
    width = s3_ref.shape[2]
    last = s3_ref.shape[1] - width
    before, after = sides_of(near_ref, far_ref, acc_ref.shape[0])
    first = acc_ref[:, :width] - times_split(before, *(s3_ref[j, :width, :] for j in range(3)))
    final = acc_ref[:, last:] - times_split(after, *(p3_ref[j, last:, :] for j in range(3)))
    return first, acc_ref[:, width:last], final


def squares(parts):
    total = None
    for part in parts:
        for i in range(0, part.shape[1], 128):
            piece = part[:, i : i + 128]
            total = piece * piece if total is None else total + piece * piece
    return total


def lane_row(total, turn, lanes):
    total = jnp.sum(total, axis=1, keepdims=True)
    rows = total.shape[0]
    row = lax.broadcasted_iota(jnp.int32, (rows, lanes), 0)
    lane = lax.broadcasted_iota(jnp.int32, (rows, lanes), 1)
    return jnp.sum(jnp.where(lane == row + turn * rows, total, 0.0), axis=0, keepdims=True)


def solve_kernel(acc_ref, near_ref, far_ref, s3_ref, p3_ref, z_ref, mix_ref, both_ref, top_ref, local_ref, norm_ref):
    parts = close_residual(acc_ref, near_ref, far_ref, s3_ref, p3_ref)
    width = s3_ref.shape[2]
    rows = acc_ref.shape[0]
    rounded = jnp.concatenate([p.astype(BF16) for p in parts], 1)
    local = dot(rounded, z_ref[...])
    local_ref[...] = local
    own_top = local[:, :width]
    mixed = times_split(split3(own_top), *(mix_ref[j] for j in range(3)))
    both_ref[:rows, :] = local[:, -width:] - mixed
    both_ref[rows:, :] = own_top
    top_ref[...] = own_top
    norm_ref[...] = squares(parts)


def norm_kernel(acc_ref, near_ref, far_ref, s3_ref, p3_ref, middle_ref, rest_ref, norm_ref, *, turn):
    first, _, final = close_residual(acc_ref, near_ref, far_ref, s3_ref, p3_ref)
    row = rest_ref[...] + lane_row(middle_ref[...] + squares((first, final)), turn, norm_ref.shape[1])
    norm_ref[...] = jnp.broadcast_to(row, norm_ref.shape)


def mix_kernel(near_ref, far_ref, chain_ref, before_ref, after_ref, mix_ref):
    even = is_even()
    width = chain_ref.shape[0]
    spikes = pl.ds(far_ref.shape[0] - width, width)
    near, far = near_ref[spikes, :], far_ref[spikes, :]
    before = choose(even, far, near)
    before_ref[...] = before
    after_ref[...] = choose(even, near, far)
    for j, part in enumerate(split3(dot(before, chain_ref[...]))):
        mix_ref[j] = part


def pair_kernel(own_ref, near_ref, second_ref, prefix_ref, whole_ref):
    right = on_right(0)
    width = own_ref.shape[0]
    own = own_ref[...].astype(F32)
    other = near_ref[pl.ds(near_ref.shape[0] - width, width), :].astype(F32)
    second = jnp.where(right, own, other).astype(BF16)
    first = jnp.where(right, other, own).astype(BF16)
    second_ref[...] = second
    row = lax.broadcasted_iota(jnp.int32, (width, width), 0)
    col = lax.broadcasted_iota(jnp.int32, (width, width), 1)
    prefix = jnp.where(right, other, jnp.where(row == col, 1.0, 0.0))
    for j, part in enumerate(split3(prefix)):
        prefix_ref[j] = part
    whole_ref[...] = dot(first, second)


def next_level(level, whole, other, prefix, second_ref, prefix_out, whole_out=None, half_out=None):
    right = on_right(level)
    second3 = split3(jnp.where(right, whole, other))
    first3 = split3(jnp.where(right, other, whole))
    for j, part in enumerate(second3):
        second_ref[j] = part
    product = None
    if whole_out is not None:
        product = times_split(first3, *second3)
        whole_out[...] = product
        if half_out is not None:
            half = half_out.shape[0]
            half_out[...] = jnp.where(is_even(), product[:half], product[half:])
    for j, part in enumerate(split3(times_split(first3, *prefix))):
        prefix_out[j] = choose(right, part, prefix[j])
    return product


def static_kernel(whole_ref, got_ref, twin_ref, prefix_ref, *outs, level):
    even = is_even()
    got, twin = got_ref[...], twin_ref[...]
    other = jnp.concatenate([jnp.where(even, twin, got), jnp.where(even, got, twin)], 0)
    next_level(level, whole_ref[...], other, parts_of(prefix_ref), *outs)


def chip_kernel(whole_ref, got_ref, twin_ref, prefix_ref, *outs):
    even = is_even()
    got, twin = got_ref[...], twin_ref[...]
    other = dot(choose(even, twin, got), choose(even, got, twin))
    next_level(1, whole_ref[...], other, parts_of(prefix_ref), *outs)


def merged(right, total, got, matrix):
    first = split3(jnp.where(right, got, total))
    product = times_split(first, *matrix) if isinstance(matrix, list) else times_exact(first, matrix)
    return product + jnp.where(right, total, got)


def parts_of(ref):
    return [ref[j] for j in range(3)]


def carry_step(level, values, reach_ref):
    return jnp.where(on_right(level), times_split(split3(values), *parts_of(reach_ref)), 0.0)


def sent_on(level, total, second_ref, carried_ref):
    product = times_split(split3(total), *parts_of(second_ref))
    carried_ref[...] = jnp.where(on_right(level), total, product)


def level0_kernel(both_ref, got_ref, second_ref, total_ref, carry_ref):
    right = on_right(0)
    rows = total_ref.shape[0]
    total, got = both_ref[:rows, :], got_ref[:rows, :]
    carry_ref[...] = jnp.where(right, got, 0.0)
    total_ref[...] = merged(right, total, got, second_ref[...])


def level0_wide_kernel(both_ref, got_ref, second_ref, next_ref, total_ref, carry_ref, carried_ref):
    level0_kernel(both_ref, got_ref, second_ref, total_ref, carry_ref)
    sent_on(1, total_ref[...], next_ref, carried_ref)


def level_kernel(total_ref, got_ref, second_ref, total_out, *, level):
    total_out[...] = merged(on_right(level), total_ref[...], got_ref[...], parts_of(second_ref))


def carry_kernel(got_ref, carry_ref, reach_ref, carry_out, *, level):
    carry_out[...] = carry_ref[...] + carry_step(level, got_ref[...], reach_ref)


def wide_kernel(total_ref, carried_ref, got_ref, low_ref, cross_ref, second_ref, second2_ref, *rest, level):
    right, right2 = on_right(level), on_right(level + 1)
    got, low = got_ref[...], low_ref[...] + cross_ref[...]
    passed = times_split(split3(got), *parts_of(second_ref))
    pair = jnp.where(right, passed + total_ref[...], carried_ref[...] + got)
    total = merged(right2, pair, low, parts_of(second2_ref))
    if len(rest) == 1:
        rest[0][...] = total
    else:
        next_ref, total_out, carried_out = rest
        total_out[...] = total
        sent_on(level + 2, total, next_ref, carried_out)


def wide_carry_kernel(got_ref, low_ref, cross_ref, carry_ref, reach_ref, reach2_ref, carry_out, *, level):
    step = carry_step(level, got_ref[...], reach_ref) + carry_step(level + 1, low_ref[...] + cross_ref[...], reach2_ref)
    carry_out[...] = carry_ref[...] + step


def tips_kernel(*refs, level, wide):
    gots, refs = refs[: 3 if wide else 1], refs[3 if wide else 1 :]
    reaches, refs = refs[: 2 if wide else 1], refs[2 if wide else 1 :]
    carry_ref, near_ref, far_ref, local_ref, x_ref, u_ref, l_ref, before_ref, after_ref, chain_ref = refs[:10]
    top_out, previous_out, near_out, far_out = refs[10:]
    even = is_even()
    rows, width = carry_ref.shape
    carry = carry_ref[...] + carry_step(level, gots[0][...], reaches[0])
    if wide:
        carry = carry + carry_step(level + 1, gots[1][...] + gots[2][...], reaches[1])
    own_top = local_ref[:, :width]
    own_bottom = local_ref[:, -width:]
    next_top = jnp.where(even, near_ref[rows:, :], far_ref[...])
    offset = own_bottom - times_exact(split3(next_top), u_ref[:, -width:])
    previous = carry - times_exact(split3(own_top), before_ref[...])
    bottom = offset + times_exact(split3(previous), chain_ref[...])
    top = (next_top - times_exact(split3(bottom), after_ref[...])).astype(BF16)
    previous = previous.astype(BF16)
    top_out[...] = top
    previous_out[...] = previous

    def updated(columns):
        change = local_ref[:, columns] - dot(top, u_ref[:, columns]) - dot(previous, l_ref[:, columns])
        return x_ref[:, columns] + change

    size = x_ref.shape[1]
    first = updated(slice(0, width))
    final = updated(slice(size - width, size))
    near_out[...] = jnp.where(even, final, first)
    far_out[...] = jnp.where(even, first, final)


def update_kernel(top_ref, previous_ref, local_ref, x_ref, u_ref, l_ref, b_ref, d3_ref, s3_ref, p3_ref, *refs):
    x_out, acc_ref = refs[-2:] if len(refs) == 2 else refs[-4:-2]
    change = local_ref[...] - dot(top_ref[...], u_ref[...]) - dot(previous_ref[...], l_ref[...])
    x_out[...] = x_ref[...] + change
    local_part(b_ref, x_out, d3_ref, s3_ref, p3_ref, acc_ref)
    if len(refs) > 2:
        norms, middle_ref, row_ref = refs[:-4], refs[-2], refs[-1]
        width = d3_ref.shape[2]
        middle_ref[...] = squares((acc_ref[:, width : acc_ref.shape[1] - width],))
        row_ref[...] = sum(lane_row(ref[...], turn, row_ref.shape[1]) for turn, ref in enumerate(norms))


def finish_kernel(gathered_ref, out_ref, *, total):
    sums = jnp.sqrt(jnp.sum(gathered_ref[...], axis=0, keepdims=True) / total)
    rows = out_ref.shape[1]
    for turn in range(out_ref.shape[0]):
        out_ref[pl.ds(turn, 1), :] = sums[:, turn * rows : (turn + 1) * rows]


def body(
    right_sides,
    initial,
    diag_blocks,
    sub_blocks,
    super_blocks,
    local_inverse,
    upper_spikes,
    lower_spikes,
):
    width = diag_blocks.shape[1]
    rows, size = right_sides.shape
    count = lax.axis_size(AXIS)
    levels = (count - 1).bit_length()
    tip = ((rows, width), F32)
    low_tip = ((rows, width), BF16)
    square = ((width, width), F32)
    low_square = ((width, width), BF16)
    triple = ((3, width, width), BF16)
    half = ((width // 2, width), F32)
    wide = ((rows, size), F32)
    big = ((3, size, width), BF16)
    lanes = -(-rows * (ITERS + 1) // 128) * 128

    near_pack, far_pack, chain = kernel_call(
        payload_kernel,
        [((3 * rows + 2 * width, width), BF16), ((3 * rows + width, width), BF16), low_square],
        (initial,), (upper_spikes,), (lower_spikes,),
    )
    near = exchange(near_pack, 1)
    far = across(far_pack)
    acc, right_sides, solution, d3, s3, p3, local_inverse, upper_spikes, lower_spikes = kernel_call(
        first_local_kernel,
        [wide, wide, wide, big, big, big, (local_inverse.shape, BF16), (upper_spikes.shape, BF16), (lower_spikes.shape, BF16)],
        *((a,) for a in (right_sides, initial, diag_blocks, sub_blocks, super_blocks, local_inverse, upper_spikes, lower_spikes)),
        micros=3,
    )
    before, after, mix = kernel_call(mix_kernel, [low_square, low_square, triple], near, far, chain)

    def swap(values, distance):
        return exchange(values, distance | 1)

    second, prefix, whole = kernel_call(pair_kernel, [low_square, triple, square], chain, near)
    seconds, reaches = [second], [None, prefix]
    for level in range(1, levels - 1):
        got = swap(chain if level == 1 else piece, 1 << level)
        twin = swap(got, 1)
        kernel = chip_kernel if level == 1 else functools.partial(static_kernel, level=level)
        second, prefix, *rest = kernel_call(
            kernel, [triple, triple] + [square, half] * (level < levels - 2), whole, got, twin, prefix, micros=1
        )
        if rest:
            whole, piece = rest
        seconds.append(second)
        reaches.append(prefix)

    norms = []
    for turn in range(ITERS):
        both, own_top, local, norm = kernel_call(
            solve_kernel, [((2 * rows, width), F32), tip, wide, ((rows, 128), F32)],
            acc, near, far, s3, p3, local_inverse, mix, micros=0.8,
        )
        norms.append(norm)
        swapped = swap(both, 1)
        far_top = across(own_top)
        groups = [(0, 1)]
        while sum(groups[-1]) < levels:
            level = sum(groups[-1])
            groups.append((level, 2 if (turn > 0 or level == 1) and level + 2 <= levels else 1))
        carried = None
        for i, (level, size_of) in enumerate(groups[:-1]):
            after_size = groups[i + 1][1]
            outs = [tip, tip] + [tip] * (after_size == 2)
            following = [seconds[level + size_of]] if after_size == 2 else []
            if level == 0:
                kernel = level0_wide_kernel if after_size == 2 else level0_kernel
                total, carry, *more = kernel_call(kernel, outs, both, swapped, seconds[0], *following)
            elif size_of == 1:
                got = swap(total, 1 << level)
                total, *more = kernel_call(
                    functools.partial(level_kernel, level=level), [tip], total, got, seconds[level]
                )
                carry = kernel_call(functools.partial(carry_kernel, level=level), [tip], got, carry, reaches[level])[0]
            else:
                step = 1 << level
                got = swap(total, step)
                low = swap(carried, 2 * step)
                cross = swap(carried, 3 * step)
                total, *more = kernel_call(
                    functools.partial(wide_kernel, level=level), outs[1:], total, carried, got, low, cross,
                    seconds[level], seconds[level + 1], *following,
                )
                carry = kernel_call(
                    functools.partial(wide_carry_kernel, level=level), [tip],
                    got, low, cross, carry, reaches[level], reaches[level + 1],
                )[0]
            carried = more[0] if more else None
        level, size_of = groups[-1]
        gots = [swap(total, 1 << level)]
        if size_of == 2:
            gots.append(swap(carried, 2 << level))
            gots.append(swap(carried, 3 << level))
        top, previous, near, far = kernel_call(
            functools.partial(tips_kernel, level=level, wide=size_of == 2), [low_tip, low_tip, tip, tip],
            *gots, *reaches[level : level + size_of], carry, swapped, far_top, local, solution, upper_spikes, lower_spikes,
            before, after, chain, micros=1,
        )
        near = exchange(near, 1)
        far = across(far)
        final = turn == ITERS - 1
        solution, acc, *sums = kernel_call(
            update_kernel, [wide, wide] + [((rows, 128), F32), ((1, lanes), F32)] * final,
            top, previous, local, solution, upper_spikes, lower_spikes, right_sides, d3, s3, p3, *(norms if final else ()),
            micros=1,
        )
    mine = kernel_call(
        functools.partial(norm_kernel, turn=ITERS), [((count, lanes), F32)], acc, near, far, s3, p3, *sums
    )[0]
    gathered = lax.all_to_all(mine, AXIS, 0, 0, tiled=True)
    result = pl.pallas_call(
        functools.partial(finish_kernel, total=size * count), out_shape=jax.ShapeDtypeStruct((ITERS + 1, rows), F32),
        compiler_params=pltpu.CompilerParams(vmem_limit_bytes=16 * 2**20),
    )(gathered)
    return solution, result


def solution(mesh):
    return jax.shard_map(
        body,
        mesh=mesh,
        in_specs=(
            P(None, AXIS),
            P(None, AXIS),
            P(AXIS, None),
            P(AXIS, None),
            P(AXIS, None),
            P(AXIS, None),
            P(None, AXIS),
            P(None, AXIS),
        ),
        out_specs=(P(None, AXIS), P()),
        check_vma=False,
    )
```
